32 devices in a mesh: replica: 4 (over y, core), fsdp: 8 (over z, x).
Axes of the slice: x: 2, y: 2, z: 4, core: 2. Of those that a mesh axis runs over, the one named last changes fastest.
Arguments:
- layer_input: bfloat16 [2, 4096, 4096], P(None, ('replica', 'fsdp')), may hold values from -6 to 6
- queries: bfloat16 [2, 4096, 4096], P(None, ('replica', 'fsdp')), may hold values from -100 to 100
- keys: bfloat16 [2, 4096, 512], P(None, ('replica', 'fsdp')), may hold values from -8 to 8
- targets: bfloat16 [2, 4096, 4096], P(None, ('replica', 'fsdp')), may hold values from -6 to 6
- value_weight: float32 [4096, 512], P('fsdp'), may hold values from -6 to 6
- outer_momentum: float32 [4096, 512], P('fsdp'), may hold values from -0.6 to 0.6
Outputs:
- new_weight: float32 [4096, 512], P('fsdp')
- new_momentum: float32 [4096, 512], P('fsdp')
The draws below stay inside these ranges and needn't reach their ends.
All inputs are finite; a program needn't handle non-finite values.
Results may differ from the reference program's by a relative error of at most 0.0017.
Values may be sent and summed in bfloat16 or wider, within the bound.
A program may use at most 64 MiB of HBM per device.

```python
import math
import jax
import jax.numpy as jnp
from jax import lax

D = 4096
QH = 32
KVH = 4
HD = 128
STEPS = 2
TOK_DEV = 128
TOKENS = 4096
N_REPLICA = 4
N_FSDP = 8


def attention_pair(seed_key):
    base = jax.random.fold_in(seed_key, 911)
    key_query, key_key = jax.random.split(base, 2)
    sequences = TOKENS // TOK_DEV
    group_size = QH // KVH
    key_rows = jax.random.normal(key_key, (STEPS, sequences, TOK_DEV, KVH, HD), jnp.float32)
    query_rows = jax.random.normal(key_query, (STEPS, sequences, TOK_DEV, KVH, group_size, HD), jnp.float32)
    query_rows = jnp.clip(query_rows, -100.0, 100.0).reshape(STEPS, TOKENS, QH * HD)
    key_rows = jnp.clip(key_rows, -8.0, 8.0).reshape(STEPS, TOKENS, KVH * HD)
    return (query_rows, key_rows)


def draw_queries(key, part):
    return attention_pair(key)[0].astype(jnp.bfloat16)


def draw_keys(key, part):
    return attention_pair(key)[1].astype(jnp.bfloat16)


def shard_levels(key, shape, cuts, least, high):
    loudness, own = 1.0, jax.random.fold_in(key, 6)
    for dim, blocks in cuts:
        heights = jnp.exp(jax.random.uniform(jax.random.fold_in(own, dim), (blocks,), jnp.float32, least / len(cuts), high / len(cuts)))
        loudness = loudness * jnp.repeat(heights, shape[dim] // blocks).reshape([-1 if axis == dim else 1 for axis in range(len(shape))])
    return loudness


def normal_values(stream_key, extent, spread, bound, shards=(), kind=jnp.bfloat16):
    result = spread * jax.random.normal(stream_key, extent, jnp.float32)
    if shards:
        result = result * shard_levels(stream_key, extent, shards, -0.22, 0.18)
    return jnp.clip(result, -bound, bound).astype(kind)


def setup_inputs(seed: int = 0) -> dict:
    arg_keys = jax.random.split(jax.random.key(seed), 7)
    return {
        "layer_input": normal_values(arg_keys[0], (STEPS, TOKENS, D), 1.0, 6.0, ((1, 32),)),
        "queries": draw_queries(jax.random.fold_in(arg_keys[6], 71), 0),
        "keys": draw_keys(jax.random.fold_in(arg_keys[6], 71), 0),
        "targets": normal_values(arg_keys[3], (STEPS, TOKENS, QH * HD), 1.0, 6.0, ((1, 32),)),
        "value_weight": normal_values(arg_keys[4], (D, KVH * HD), 1.0, 6.0, ((0, 8),), jnp.float32),
        "outer_momentum": normal_values(arg_keys[5], (D, KVH * HD), 0.1, 0.6, ((0, 8),), jnp.float32),
    }


beta_one = 0.9
beta_two = 0.95
inner_rate = 0.05
decay_rate = 0.1
outer_rate = 0.7
outer_mu = 0.9

def sequence_grad(query_rows, key_rows, values, target_rows):
    group_size = QH // KVH
    length = query_rows.shape[0]
    query_heads = query_rows.astype(jnp.float32).reshape(length, KVH, group_size, HD)
    key_heads = key_rows.astype(jnp.float32).reshape(length, KVH, HD)
    scores = jnp.einsum('qgjd,kgd->gjqk', query_heads, key_heads) / math.sqrt(HD)
    causal = jnp.arange(length)[:, None] >= jnp.arange(length)[None, :]
    scores = jnp.where(causal, scores, -1e+30)
    highest = lax.optimization_barrier(jnp.max(scores, axis=-1, keepdims=True))
    expd = jnp.exp(scores - highest)
    attention = (expd / lax.optimization_barrier(jnp.sum(expd, axis=-1, keepdims=True))).astype(jnp.bfloat16)
    attn_wide = attention.astype(jnp.float32)
    value_heads = values.astype(jnp.float32).reshape(length, KVH, HD)
    attended = jnp.einsum('gjqk,kgd->qgjd', attn_wide, value_heads).reshape(length, QH * HD)
    out_grad = ((attended - target_rows.astype(jnp.float32)) / (TOK_DEV * N_FSDP)).astype(jnp.bfloat16)
    grad_heads = out_grad.astype(jnp.float32).reshape(length, KVH, group_size, HD)
    value_grad = jnp.einsum('gjqk,qgjd->kgd', attn_wide, grad_heads).reshape(length, KVH * HD)
    return value_grad.astype(jnp.bfloat16)

def replica_round(value_weight, layer_input, queries, keys, targets, replica):
    tok_rep = TOK_DEV * N_FSDP
    adam_floor = math.sqrt(QH // KVH / (tok_rep * D))
    first_row = replica * tok_rep
    weights_now = value_weight
    moment_one = jnp.zeros_like(value_weight)
    moment_two = jnp.zeros_like(value_weight)
    for step_index in range(STEPS):
        inputs = layer_input[step_index, first_row:first_row + tok_rep]
        weights_bf = weights_now.astype(jnp.bfloat16)
        values = (jnp.dot(inputs, weights_bf, preferred_element_type=jnp.float32) / math.sqrt(D)).astype(jnp.bfloat16)
        query_seq = queries[step_index, first_row:first_row + tok_rep].reshape(N_FSDP, TOK_DEV, QH * HD)
        key_seq = keys[step_index, first_row:first_row + tok_rep].reshape(N_FSDP, TOK_DEV, KVH * HD)
        value_seq = values.reshape(N_FSDP, TOK_DEV, KVH * HD)
        target_seq = targets[step_index, first_row:first_row + tok_rep].reshape(N_FSDP, TOK_DEV, QH * HD)
        value_grad = lax.map(lambda group: sequence_grad(group[0], group[1], group[2], group[3]), (query_seq, key_seq, value_seq, target_seq))
        value_grad = value_grad.reshape(tok_rep, KVH * HD)
        gradient = jnp.dot(inputs.T, value_grad, preferred_element_type=jnp.float32) / math.sqrt(D)
        moment_one = beta_one * moment_one + (1.0 - beta_one) * gradient
        moment_two = beta_two * moment_two + (1.0 - beta_two) * gradient * gradient
        corrected_one = moment_one / (1.0 - beta_one ** (step_index + 1))
        corrected_two = moment_two / (1.0 - beta_two ** (step_index + 1))
        weights_now = weights_now - inner_rate * (corrected_one / (jnp.sqrt(corrected_two) + adam_floor) + decay_rate * weights_now)
    return weights_now

def reference(layer_input, queries, keys, targets, value_weight, outer_momentum):
    total_delta = jnp.zeros_like(value_weight)
    for replica in range(N_REPLICA):
        total_delta = total_delta + (value_weight - replica_round(value_weight, layer_input, queries, keys, targets, replica))
    mean_delta = total_delta / N_REPLICA
    new_momentum = outer_mu * outer_momentum + mean_delta
    new_weight = value_weight - outer_rate * (mean_delta + outer_mu * new_momentum)
    return (new_weight, new_momentum)
```

```python
import math

import jax
import jax.numpy as jnp
from jax import lax
from jax.experimental import pallas as pl
from jax.experimental.pallas import tpu as pltpu
from jax.sharding import PartitionSpec as P

D = 4096
QH = 32
KVH = 4
HD = 128


beta_one = 0.9
beta_two = 0.95
inner_rate = 0.05
decay_rate = 0.1
outer_rate = 0.7
outer_mu = 0.9


def plain_shards(layer_input, queries, keys, targets, value_weight, outer_momentum):
    inner_steps = layer_input.shape[0]
    length = layer_input.shape[1]
    columns = value_weight.shape[1]
    fsdp_count = lax.axis_size("fsdp")
    replicas = lax.axis_size("replica")
    tok_rep = length * fsdp_count
    group_size = QH // KVH
    adam_floor = math.sqrt(group_size / (tok_rep * D))
    by_features = lax.all_to_all(layer_input, "fsdp", split_axis=2, concat_axis=1, tiled=True)
    causal = jnp.arange(length)[:, None] >= jnp.arange(length)[None, :]
    weights_now = value_weight
    moment_one = jnp.zeros_like(value_weight)
    moment_two = jnp.zeros_like(value_weight)
    for step_index in range(inner_steps):
        inputs = layer_input[step_index]
        shard_bf = weights_now.astype(jnp.bfloat16)
        product = jnp.dot(
            inputs,
            lax.all_gather(shard_bf, "fsdp", axis=0, tiled=True),
            preferred_element_type=jnp.float32,
        )
        values = (product / math.sqrt(D)).astype(jnp.bfloat16)
        query_heads = queries[step_index].reshape(length, KVH, group_size, HD)
        key_heads = keys[step_index].reshape(length, KVH, HD)
        scores = jnp.einsum(
            "qgjd,kgd->gjqk", query_heads, key_heads, preferred_element_type=jnp.float32
        ) / math.sqrt(HD)
        scores = jnp.where(causal, scores, -1e30)
        highest = jnp.max(scores, axis=-1, keepdims=True)
        expd = jnp.exp(scores - highest)
        attention = (expd / jnp.sum(expd, axis=-1, keepdims=True)).astype(jnp.bfloat16)
        attended = jnp.einsum(
            "gjqk,kgd->qgjd",
            attention,
            values.reshape(length, KVH, HD),
            preferred_element_type=jnp.float32,
        ).reshape(length, QH * HD)
        out_grad = ((attended - targets[step_index].astype(jnp.float32)) / tok_rep).astype(
            jnp.bfloat16
        )
        value_grad = (
            jnp.einsum(
                "gjqk,qgjd->kgd",
                attention,
                out_grad.reshape(length, KVH, group_size, HD),
                preferred_element_type=jnp.float32,
            )
            .reshape(length, columns)
            .astype(jnp.bfloat16)
        )
        step_features = by_features[step_index]
        gradient = lax.dot_general(
            step_features,
            lax.all_gather(value_grad, "fsdp", axis=0, tiled=True),
            (((0,), (0,)), ((), ())),
            preferred_element_type=jnp.float32,
        ) / math.sqrt(D)
        moment_one = beta_one * moment_one + (1.0 - beta_one) * gradient
        moment_two = beta_two * moment_two + (1.0 - beta_two) * gradient * gradient
        corrected_one = moment_one / (1.0 - beta_one ** (step_index + 1))
        corrected_two = moment_two / (1.0 - beta_two ** (step_index + 1))
        weights_now = weights_now - inner_rate * (
            corrected_one / (jnp.sqrt(corrected_two) + adam_floor) + decay_rate * weights_now
        )
    total_delta = lax.psum(value_weight - weights_now, "replica")
    mean_delta = total_delta / replicas
    new_momentum = outer_mu * outer_momentum + mean_delta
    new_weight = value_weight - outer_rate * (mean_delta + outer_mu * new_momentum)
    return (new_weight, new_momentum)


MESH = pl.DeviceIdType.MESH


def round_kernel(
    x_ref,
    q_ref,
    k_ref,
    t_ref,
    w_ref,
    mean_ref,
    feat,
    q_buf,
    k_buf,
    t_buf,
    w_buf,
    wb,
    w_now,
    mat,
    base,
    pair_out,
    pair_in,
    red_out,
    red_in,
    vgrad,
    grad,
    first_update,
    sy_out,
    sy_in,
    s_own,
    halves,
    tot_mine,
    tot_other,
    in_s,
    in_r,
    w_s,
    w_r,
    mat_s,
    mat_r,
    pair_s,
    pair_r,
    red_s,
    red_r,
    ag_s,
    ag_r,
    fw_s,
    fw_r,
    fin_s,
    fin_r,
    load_s,
):
    steps, length, _ = x_ref.shape
    rows, columns = w_ref.shape
    parts = 2
    width = columns // parts
    wide = [slice(p * width, (p + 1) * width) for p in range(parts)]
    heads = columns // HD
    group = QH // KVH
    quad = 4 * length
    tok_rep = 2 * quad
    adam_floor = math.sqrt(group / (tok_rep * D))
    shrink = 1.0 - inner_rate * decay_rate
    me = lax.axis_index("fsdp")
    rep = lax.axis_index("replica")
    x = me % 2
    low = (me // 2) % 2
    half = me // 4
    y = rep // 2
    core = rep % 2
    sel = (half + core) % 2
    far = sel == 1
    near = sel == 0

    def device(h, l, xx, yy, cc):
        return {"replica": yy * 2 + cc, "fsdp": (h * 2 + l) * 2 + xx}

    core_peer = device(half, low, x, y, 1 - core)
    y_peer = device(half, low, x, 1 - y, core)
    partner = device(core, low, x, y, half)

    def mate(a, b):
        return device(half, (low + a) % 2, (x + b) % 2, y, core)

    def offset(a, b):
        return (((low + a) % 2) * 2 + (x + b) % 2) * length

    quads = [(1, 1), (0, 1), (1, 0), (0, 0)]
    mine = pl.multiple_of(core * quad, quad)
    theirs = pl.multiple_of((1 - core) * quad, quad)

    def at(start, size):
        return pl.ds(pl.multiple_of(start, 32), size)

    loads = {}

    def load(i, src, dst):
        loads[i] = pltpu.make_async_copy(src, dst, load_s.at[i])
        loads[i].start()

    barrier = pltpu.get_barrier_semaphore()
    count = 0
    for dh in range(2):
        for dl in range(2):
            for dx in range(2):
                for dc in range(2):
                    if dh + dl + dx + dc:
                        peer = device(
                            (half + dh) % 2, (low + dl) % 2, (x + dx) % 2, y, (core + dc) % 2
                        )
                        pl.semaphore_signal(barrier, inc=1, device_id=peer, device_id_type=MESH)
                        count += 1
    pl.semaphore_signal(barrier, inc=1, device_id=y_peer, device_id_type=MESH)
    load(0, w_ref, w_buf)
    load(1, q_ref, q_buf)
    load(2, k_ref, k_buf)
    load(3, t_ref, t_buf)
    pl.semaphore_wait(barrier, count + 1)

    pending, far_pending, near_pending = [], [], []

    def remote(src, dst, ssem, rsem, peer):
        return pltpu.make_async_remote_copy(
            src_ref=src,
            dst_ref=dst,
            send_sem=ssem,
            recv_sem=rsem,
            device_id=peer,
            device_id_type=MESH,
        )

    def send(*args):
        copy = remote(*args)
        copy.start()
        pending.append(copy)
        return copy

    def send_if(cond, keep, *args):
        copy = remote(*args)

        @pl.when(cond)
        def _():
            copy.start()

        keep.append(copy)
        return copy

    def wait_if(cond, copy):
        @pl.when(cond)
        def _():
            copy.wait_recv()

    def send_inputs(s, picks):
        for a, b, dc in picks:
            l2, x2, c2 = (low + a) % 2, (x + b) % 2, (core + dc) % 2
            i = a * 4 + b * 2 + dc
            src = x_ref.at[
                s, :, pl.ds(pl.multiple_of(((c2 * 2 + l2) * 2 + x2) * rows, 128), rows)
            ]
            dst = feat.at[s, at(me * length, length)]
            args = (src, dst, in_s.at[s, i], in_r.at[s, me], device(core, l2, x2, y, c2))
            if i:
                send(*args)
            else:
                send_if(far, far_pending, *args)

                @pl.when(near)
                def _():
                    pltpu.make_async_copy(src, dst, in_r.at[s, me]).start()

    def wait_input(s, j):
        slot = feat.at[s, at(j * length, length)]
        remote(slot, slot, in_s.at[s, 0], in_r.at[s, j], core_peer).wait_recv()

    causal = lax.broadcasted_iota(jnp.int32, (length, length), 0) >= lax.broadcasted_iota(
        jnp.int32, (length, length), 1
    )

    def attention_of(s):
        def one(g, carry):
            keys = k_buf[s, :, pl.ds(pl.multiple_of(g * HD, HD), HD)]
            both = jnp.zeros((length, length + HD), jnp.float32)
            for j in range(group):
                cols = pl.ds(pl.multiple_of((g * group + j) * HD, HD), HD)
                scores = lax.dot_general(
                    q_buf[s, :, cols],
                    keys,
                    (((1,), (1,)), ((), ())),
                    preferred_element_type=jnp.float32,
                ) / math.sqrt(HD)
                scores = jnp.where(causal, scores, -1e30)
                highest = jnp.max(scores, axis=-1, keepdims=True)
                expd = jnp.exp(scores - highest)
                att = (expd / jnp.sum(expd, axis=-1, keepdims=True)).astype(jnp.bfloat16)
                both += lax.dot_general(
                    att,
                    jnp.concatenate([att, t_buf[s, :, cols]], axis=1),
                    (((0,), (0,)), ((), ())),
                    preferred_element_type=jnp.float32,
                )
            mat[0, s, g] = both[:, :length].astype(jnp.bfloat16)
            base[0, s, g] = both[:, length:].astype(jnp.bfloat16)
            return carry

        lax.fori_loop(0, heads, one, 0)
        first = send_if(
            far, far_pending, mat.at[0, s], mat.at[1, s], mat_s.at[s, 0], mat_r.at[s, 0], partner
        )
        second = send_if(
            far, far_pending, base.at[0, s], base.at[1, s], mat_s.at[s, 1], mat_r.at[s, 1], partner
        )
        return first, second

    chunk = 32

    def over(start, size, body):
        def step(i, carry):
            body(i * chunk)
            return carry

        lax.fori_loop(0, size // chunk, step, 0)

    order = [(a, b, dc) for a, b in quads for dc in (1, 0)]
    send_inputs(0, order[:4])
    loads[0].wait()

    def cast_weights(r):
        wb[0, at(r, chunk), :] = w_buf[at(r, chunk), :].astype(jnp.bfloat16)

    over(0, rows, cast_weights)
    mid = rows // 2
    w_mine = at(y * mid, mid)
    w_cross = send_if(
        far, far_pending, wb.at[0, w_mine], wb.at[1, w_mine], w_s.at[0], w_r.at[0], partner
    )
    send_inputs(0, order[4:])
    for i in (1, 2, 3):
        loads[i].wait()
    mats = [attention_of(0)]
    wait_if(far, w_cross)
    w_relay = send_if(
        far, far_pending, wb.at[1, w_mine], wb.at[1, w_mine], w_s.at[1], w_r.at[1], y_peer
    )
    later = {s: list(order) for s in range(1, steps)}
    for s in range(1, steps):
        send_inputs(s, later[s][:2])
        later[s] = later[s][2:]
        mats.append(attention_of(s))
    wait_if(far, w_relay)

    def weights(s, p):
        return wb[sel, :, wide[p]] if s == 0 else w_now[:, wide[p]]

    for s in range(steps):
        def feed(k):
            if s + 1 < steps:
                send_inputs(s + 1, later[s + 1][:k])
                later[s + 1] = later[s + 1][k:]

        for a, b in quads:
            wait_input(s, (1 - core) * 4 + ((low + a) % 2) * 2 + (x + b) % 2)
        pairs = {}
        for a in (1, 0):
            start = ((low + a) % 2) * 2 * length
            span = at(start, 2 * length)
            for p in range(parts):
                part = jnp.dot(
                    feat[s, at(theirs + start, 2 * length)],
                    weights(s, p),
                    preferred_element_type=jnp.float32,
                )
                pair_out[s, span, wide[p]] = part.astype(jnp.bfloat16)
                pairs[a, p] = send(
                    pair_out.at[s, span, wide[p]],
                    pair_in.at[s, span, wide[p]],
                    pair_s.at[s, a, p],
                    pair_r.at[s, a, p],
                    core_peer,
                )
        for a, b in quads:
            wait_input(s, core * 4 + ((low + a) % 2) * 2 + (x + b) % 2)
        reds = {}
        for p in range(parts):
            for a in (1, 0):
                start = ((low + a) % 2) * 2 * length
                span = at(start, 2 * length)
                own = jnp.dot(
                    feat[s, at(mine + start, 2 * length)],
                    weights(s, p),
                    preferred_element_type=jnp.float32,
                )
                pairs[a, p].wait_recv()
                own = own + pair_in[s, span, wide[p]].astype(jnp.float32)
                red_out[s, span, wide[p]] = own.astype(jnp.bfloat16)
                for b in (1, 0):
                    if a + b:
                        reds[a, b, p] = send(
                            red_out.at[s, at(offset(a, b), length), wide[p]],
                            red_in.at[s, a * 2 + b, :, wide[p]],
                            red_s.at[s, a * 2 + b, p],
                            red_r.at[s, a * 2 + b, p],
                            mate(a, b),
                        )
        feed(2)
        for copy in mats[s]:
            wait_if(far, copy)
        gathers, passes = {}, {}
        slot = at(me_slot(core, low, x) * length, length)
        for p in range(parts):
            summed = red_out[s, at(offset(0, 0), length), wide[p]].astype(jnp.float32)
            for a, b in quads[:3]:
                reds[a, b, p].wait_recv()
                summed = summed + red_in[s, a * 2 + b, :, wide[p]].astype(jnp.float32)
            values = (summed / math.sqrt(D)).astype(jnp.bfloat16)
            for i in range(width // HD):
                g = p * (width // HD) + i
                part = values[:, i * HD : (i + 1) * HD]
                vg = jnp.dot(mat[sel, s, g], part, preferred_element_type=jnp.float32)
                vg = (vg - base[sel, s, g].astype(jnp.float32)) / tok_rep
                vgrad[s, slot, g * HD : (g + 1) * HD] = vg.astype(jnp.bfloat16)
            block = vgrad.at[s, slot, wide[p]]
            for a, b in quads[:3]:
                i = a * 2 + b
                gathers[a, b, p] = send(
                    block, block, ag_s.at[s, i, p], ag_r.at[s, i, p], mate(a, b)
                )
            passes[0, 0, p] = send(
                block, block, fw_s.at[s, 0, p], fw_r.at[s, 0, p], core_peer
            )
        feed(2)

        def add_quad(start, p, first):
            term = lax.dot_general(
                feat[s, at(start, quad)],
                vgrad[s, at(start, quad), wide[p]],
                (((0,), (0,)), ((), ())),
                preferred_element_type=jnp.float32,
            )
            if first:
                grad[s, :, wide[p]] = term
            else:
                grad[s, :, wide[p]] += term

        for p in range(parts):
            for a, b in quads[2::-1]:
                gathers[a, b, p].wait_recv()
                i = a * 2 + b
                block = vgrad.at[s, at(mine + offset(a, b), length), wide[p]]
                passes[a, b, p] = send(
                    block, block, fw_s.at[s, i, p], fw_r.at[s, i, p], core_peer
                )
            add_quad(mine, p, True)
        feed(8)
        for p in range(parts):
            for a, b in quads:
                passes[a, b, p].wait_recv()
            add_quad(theirs, p, False)

        def adam(r, keep):
            c = at(r, chunk)
            one, two = 0.0, 0.0
            for i in range(s + 1):
                gradient = grad[i, c, :] / math.sqrt(D)
                one = beta_one * one + (1.0 - beta_one) * gradient
                two = beta_two * two + (1.0 - beta_two) * gradient * gradient
            fixed_one = one / (1.0 - beta_one ** (s + 1))
            fixed_two = two / (1.0 - beta_two ** (s + 1))
            update = fixed_one / (jnp.sqrt(fixed_two) + adam_floor)
            keep(c, update)

        if s + 1 < steps:

            def keep(c, update):
                before = wb[sel, c, :].astype(jnp.float32)
                first_update[c, :] = update
                w_now[c, :] = (before * shrink - inner_rate * update).astype(jnp.bfloat16)

            over(0, rows, lambda r: adam(r, keep))

    def moved(c, update):
        return inner_rate * (shrink * first_update[c, :] + update)

    pieces = 2
    size = mid // pieces
    sub = size // 2
    firsts, seconds, thirds, fourths, fifths = [], [], [], [], []
    for p in range(pieces):

        def out_piece(r):
            def put(c, update):
                sy_out[at(p * size + r, chunk), :] = moved(c, update).astype(jnp.bfloat16)

            adam((1 - y) * mid + p * size + r, put)

        over(0, size, out_piece)
        piece = at(p * size, size)
        firsts.append(
            send(sy_out.at[piece], sy_in.at[piece], fin_s.at[0, p], fin_r.at[0, p], y_peer)
        )
    for p in range(pieces):

        def own_piece(r):
            def put(c, update):
                s_own[at(p * size + r, chunk), :] = moved(c, update)

            adam(y * mid + p * size + r, put)

        over(0, size, own_piece)
    for p in range(pieces):
        piece = at(p * size, size)
        firsts[p].wait_recv()

        def join(r):
            c = at(p * size + r, chunk)
            halves[2 * sel, c, :] = (s_own[c, :] + sy_in[c, :].astype(jnp.float32)).astype(
                jnp.bfloat16
            )

        over(0, size, join)
        seconds.append(
            send_if(
                near,
                near_pending,
                halves.at[0, piece],
                halves.at[0, piece],
                fin_s.at[1, p],
                fin_r.at[1, p],
                core_peer,
            )
        )
        thirds.append(
            send_if(
                far,
                far_pending,
                halves.at[2, piece],
                halves.at[1, piece],
                fin_s.at[2, p],
                fin_r.at[2, p],
                partner,
            )
        )
    replicas = 4
    for p in range(pieces):
        piece = at(p * size, size)
        wait_if(far, thirds[p])
        fourths.append(
            send_if(
                far,
                far_pending,
                halves.at[1, piece],
                halves.at[1, piece],
                fin_s.at[3, p],
                fin_r.at[3, p],
                core_peer,
            )
        )
        wait_if(far, seconds[p])
        wait_if(near, fourths[p])

        def total(r):
            c = at(p * size + r, chunk)
            both = (
                halves[0, c, :].astype(jnp.float32) + halves[1, c, :].astype(jnp.float32)
            ).astype(jnp.bfloat16)
            tot_mine[c, :] = both
            mean_ref[at(y * mid + p * size + r, chunk), :] = both.astype(jnp.float32) / replicas

        over(0, size, total)
        bit = at(p * size + core * sub, sub)
        fifths.append(
            send(tot_mine.at[bit], tot_other.at[bit], fin_s.at[4, p], fin_r.at[4, p], y_peer)
        )
    sixths = []
    for p in range(pieces):
        bit = at(p * size + core * sub, sub)
        fifths[p].wait_recv()
        sixths.append(
            send(tot_other.at[bit], tot_other.at[bit], fin_s.at[5, p], fin_r.at[5, p], core_peer)
        )
    for p in range(pieces):
        sixths[p].wait_recv()

        def finish(r):
            c = at(p * size + r, chunk)
            mean_ref[at((1 - y) * mid + p * size + r, chunk), :] = (
                tot_other[c, :].astype(jnp.float32) / replicas
            )

        over(0, size, finish)
    for copy in pending:
        copy.wait_send()

    @pl.when(far)
    def _():
        for copy in far_pending:
            copy.wait_send()

    @pl.when(near)
    def _():
        for copy in near_pending:
            copy.wait_send()


def me_slot(core, low, x):
    return (core * 2 + low) * 2 + x


def shards(layer_input, queries, keys, targets, value_weight, outer_momentum):
    n = lax.axis_size("fsdp")
    replicas = lax.axis_size("replica")
    rows, columns = value_weight.shape
    steps, length, _ = layer_input.shape
    if rows % 512 or columns % (2 * HD) or n != 8 or replicas != 4 or length % 128 or steps != 2:
        return plain_shards(layer_input, queries, keys, targets, value_weight, outer_momentum)
    heads = columns // HD
    bf, f32 = jnp.bfloat16, jnp.float32
    dma = pltpu.SemaphoreType.DMA
    out = jax.ShapeDtypeStruct((rows, columns), f32)
    mean_update = pl.pallas_call(
        round_kernel,
        out_shape=out,
        in_specs=[pl.BlockSpec(memory_space=pl.ANY)] * 5,
        out_specs=pl.BlockSpec(memory_space=pltpu.VMEM),
        scratch_shapes=[
            pltpu.VMEM((steps, n * length, rows), bf),
            pltpu.VMEM(queries.shape, bf),
            pltpu.VMEM(keys.shape, bf),
            pltpu.VMEM(targets.shape, bf),
            pltpu.VMEM((rows, columns), f32),
            pltpu.VMEM((2, rows, columns), bf),
            pltpu.VMEM((rows, columns), bf),
            pltpu.VMEM((2, steps, heads, length, length), bf),
            pltpu.VMEM((2, steps, heads, length, HD), bf),
            pltpu.VMEM((steps, 4 * length, columns), bf),
            pltpu.VMEM((steps, 4 * length, columns), bf),
            pltpu.VMEM((steps, 4 * length, columns), bf),
            pltpu.VMEM((steps, 4, length, columns), bf),
            pltpu.VMEM((steps, n * length, columns), bf),
            pltpu.VMEM((steps, rows, columns), f32),
            pltpu.VMEM((rows, columns), f32),
            pltpu.VMEM((rows // 2, columns), bf),
            pltpu.VMEM((rows // 2, columns), bf),
            pltpu.VMEM((rows // 2, columns), f32),
            pltpu.VMEM((3, rows // 2, columns), bf),
            pltpu.VMEM((rows // 2, columns), bf),
            pltpu.VMEM((rows // 2, columns), bf),
            dma((steps, n)),
            dma((steps, n)),
            dma((2,)),
            dma((2,)),
            dma((steps, 2)),
            dma((steps, 2)),
            dma((steps, 2, 2)),
            dma((steps, 2, 2)),
            dma((steps, 4, 2)),
            dma((steps, 4, 2)),
            dma((steps, 4, 2)),
            dma((steps, 4, 2)),
            dma((steps, 4, 2)),
            dma((steps, 4, 2)),
            dma((6, 2)),
            dma((6, 2)),
            dma((4,)),
        ],
        compiler_params=pltpu.CompilerParams(collective_id=0, has_side_effects=True),
    )(layer_input, queries, keys, targets, value_weight)
    kept = (1.0 - inner_rate * decay_rate) ** steps
    mean_delta = (1.0 - kept) * value_weight + mean_update
    new_momentum = outer_mu * outer_momentum + mean_delta
    new_weight = value_weight - outer_rate * (mean_delta + outer_mu * new_momentum)
    return (new_weight, new_momentum)


def solution(mesh):
    in_specs = (
        P(None, ("replica", "fsdp"), None),
        P(None, ("replica", "fsdp"), None),
        P(None, ("replica", "fsdp"), None),
        P(None, ("replica", "fsdp"), None),
        P("fsdp", None),
        P("fsdp", None),
    )
    out_specs = (P("fsdp", None), P("fsdp", None))
    return jax.shard_map(shards, mesh=mesh, in_specs=in_specs, out_specs=out_specs, check_vma=False)
```

```python
import math

import jax
import jax.numpy as jnp
from jax import lax
from jax.experimental import pallas as pl
from jax.experimental.pallas import tpu as pltpu
from jax.sharding import PartitionSpec as P

D = 4096
QH = 32
KVH = 4
HD = 128


beta_one = 0.9
beta_two = 0.95
inner_rate = 0.05
decay_rate = 0.1
outer_rate = 0.7
outer_mu = 0.9


def plain_shards(layer_input, queries, keys, targets, value_weight, outer_momentum):
    inner_steps = layer_input.shape[0]
    length = layer_input.shape[1]
    columns = value_weight.shape[1]
    fsdp_count = lax.axis_size("fsdp")
    replicas = lax.axis_size("replica")
    tok_rep = length * fsdp_count
    group_size = QH // KVH
    adam_floor = math.sqrt(group_size / (tok_rep * D))
    by_features = lax.all_to_all(layer_input, "fsdp", split_axis=2, concat_axis=1, tiled=True)
    causal = jnp.arange(length)[:, None] >= jnp.arange(length)[None, :]
    weights_now = value_weight
    moment_one = jnp.zeros_like(value_weight)
    moment_two = jnp.zeros_like(value_weight)
    for step_index in range(inner_steps):
        inputs = layer_input[step_index]
        shard_bf = weights_now.astype(jnp.bfloat16)
        product = jnp.dot(
            inputs,
            lax.all_gather(shard_bf, "fsdp", axis=0, tiled=True),
            preferred_element_type=jnp.float32,
        )
        values = (product / math.sqrt(D)).astype(jnp.bfloat16)
        query_heads = queries[step_index].reshape(length, KVH, group_size, HD)
        key_heads = keys[step_index].reshape(length, KVH, HD)
        scores = jnp.einsum(
            "qgjd,kgd->gjqk", query_heads, key_heads, preferred_element_type=jnp.float32
        ) / math.sqrt(HD)
        scores = jnp.where(causal, scores, -1e30)
        highest = jnp.max(scores, axis=-1, keepdims=True)
        expd = jnp.exp(scores - highest)
        attention = (expd / jnp.sum(expd, axis=-1, keepdims=True)).astype(jnp.bfloat16)
        attended = jnp.einsum(
            "gjqk,kgd->qgjd",
            attention,
            values.reshape(length, KVH, HD),
            preferred_element_type=jnp.float32,
        ).reshape(length, QH * HD)
        out_grad = ((attended - targets[step_index].astype(jnp.float32)) / tok_rep).astype(
            jnp.bfloat16
        )
        value_grad = (
            jnp.einsum(
                "gjqk,qgjd->kgd",
                attention,
                out_grad.reshape(length, KVH, group_size, HD),
                preferred_element_type=jnp.float32,
            )
            .reshape(length, columns)
            .astype(jnp.bfloat16)
        )
        step_features = by_features[step_index]
        gradient = lax.dot_general(
            step_features,
            lax.all_gather(value_grad, "fsdp", axis=0, tiled=True),
            (((0,), (0,)), ((), ())),
            preferred_element_type=jnp.float32,
        ) / math.sqrt(D)
        moment_one = beta_one * moment_one + (1.0 - beta_one) * gradient
        moment_two = beta_two * moment_two + (1.0 - beta_two) * gradient * gradient
        corrected_one = moment_one / (1.0 - beta_one ** (step_index + 1))
        corrected_two = moment_two / (1.0 - beta_two ** (step_index + 1))
        weights_now = weights_now - inner_rate * (
            corrected_one / (jnp.sqrt(corrected_two) + adam_floor) + decay_rate * weights_now
        )
    total_delta = lax.psum(value_weight - weights_now, "replica")
    mean_delta = total_delta / replicas
    new_momentum = outer_mu * outer_momentum + mean_delta
    new_weight = value_weight - outer_rate * (mean_delta + outer_mu * new_momentum)
    return (new_weight, new_momentum)


MESH = pl.DeviceIdType.MESH


def round_kernel(
    x_ref,
    q_ref,
    k_ref,
    t_ref,
    w_ref,
    mean_ref,
    feat,
    q_buf,
    k_buf,
    t_buf,
    w_buf,
    wb,
    w_now,
    own_part,
    mat,
    base,
    pair_out,
    pair_in,
    red_out,
    red_in,
    vgrad,
    grad,
    first_update,
    sy_out,
    sy_in,
    s_own,
    halves,
    tot_mine,
    tot_other,
    in_s,
    in_r,
    w_s,
    w_r,
    mat_s,
    mat_r,
    pair_s,
    pair_r,
    red_s,
    red_r,
    ag_s,
    ag_r,
    fw_s,
    fw_r,
    fin_s,
    fin_r,
    load_s,
):
    steps, length, _ = x_ref.shape
    rows, columns = w_ref.shape
    parts = 2
    width = columns // parts
    wide = [slice(p * width, (p + 1) * width) for p in range(parts)]
    heads = columns // HD
    group = QH // KVH
    quad = 4 * length
    tok_rep = 2 * quad
    adam_floor = math.sqrt(group / (tok_rep * D))
    shrink = 1.0 - inner_rate * decay_rate
    me = lax.axis_index("fsdp")
    rep = lax.axis_index("replica")
    x = me % 2
    low = (me // 2) % 2
    half = me // 4
    y = rep // 2
    core = rep % 2
    sel = (half + core) % 2
    far = sel == 1
    near = sel == 0
    beside = jnp.logical_and(far, low != half)
    outer = jnp.logical_and(far, low == half)

    def device(h, l, xx, yy, cc):
        return {"replica": yy * 2 + cc, "fsdp": (h * 2 + l) * 2 + xx}

    core_peer = device(half, low, x, y, 1 - core)
    y_peer = device(half, low, x, 1 - y, core)
    partner = device(core, low, x, y, half)

    def mate(a, b):
        return device(half, (low + a) % 2, (x + b) % 2, y, core)

    def offset(a, b):
        return (((low + a) % 2) * 2 + (x + b) % 2) * length

    quads = [(1, 1), (0, 1), (1, 0), (0, 0)]

    def at(start, size):
        return pl.ds(pl.multiple_of(start, 32), size)

    loads = {}

    def load(i, src, dst):
        loads[i] = pltpu.make_async_copy(src, dst, load_s.at[i])
        loads[i].start()

    barrier = pltpu.get_barrier_semaphore()
    count = 0
    for dh in range(2):
        for dl in range(2):
            for dx in range(2):
                for dc in range(2):
                    if dh + dl + dx + dc:
                        peer = device(
                            (half + dh) % 2, (low + dl) % 2, (x + dx) % 2, y, (core + dc) % 2
                        )
                        pl.semaphore_signal(barrier, inc=1, device_id=peer, device_id_type=MESH)
                        count += 1
    for dc in range(2):
        peer = device(half, low, x, 1 - y, (core + dc) % 2)
        pl.semaphore_signal(barrier, inc=1, device_id=peer, device_id_type=MESH)
    load(0, w_ref, w_buf)
    load(1, q_ref, q_buf)
    load(2, k_ref, k_buf)
    load(3, t_ref, t_buf)
    pl.semaphore_wait(barrier, count + 2)

    pending, far_pending, near_pending = [], [], []

    def remote(src, dst, ssem, rsem, peer):
        return pltpu.make_async_remote_copy(
            src_ref=src,
            dst_ref=dst,
            send_sem=ssem,
            recv_sem=rsem,
            device_id=peer,
            device_id_type=MESH,
        )

    def send(*args):
        copy = remote(*args)
        copy.start()
        pending.append(copy)
        return copy

    def send_if(cond, keep, *args):
        copy = remote(*args)

        @pl.when(cond)
        def _():
            copy.start()

        keep.append(copy)
        return copy

    def wait_if(cond, copy):
        @pl.when(cond)
        def _():
            copy.wait_recv()

    def send_inputs(s, picks, cond=None, keep=None):
        for a, b, dc in picks:
            l2, x2, c2 = (low + a) % 2, (x + b) % 2, (core + dc) % 2
            i = a * 4 + b * 2 + dc
            src = x_ref.at[
                s, :, pl.ds(pl.multiple_of(((c2 * 2 + l2) * 2 + x2) * rows, 128), rows)
            ]
            dst = feat.at[s, at(me * length, length)]
            args = (src, dst, in_s.at[s, i], in_r.at[s, me], device(core, l2, x2, y, c2))
            if i and cond is None:
                send(*args)
            elif i:
                send_if(cond, keep, *args)
            else:
                if cond is not near:
                    send_if(far if cond is None else cond, far_pending if cond is None else keep, *args)
                if cond is None or cond is near:

                    @pl.when(near)
                    def _():
                        pltpu.make_async_copy(src, dst, in_r.at[s, me]).start()

    def wait_input(s, j):
        slot = feat.at[s, at(j * length, length)]
        remote(slot, slot, in_s.at[s, 0], in_r.at[s, j], core_peer).wait_recv()

    causal = lax.broadcasted_iota(jnp.int32, (length, length), 0) >= lax.broadcasted_iota(
        jnp.int32, (length, length), 1
    )

    def attention_of(s):
        def one(g, carry):
            keys = k_buf[s, :, pl.ds(pl.multiple_of(g * HD, HD), HD)]
            both = jnp.zeros((length, length + HD), jnp.float32)
            for j in range(group):
                cols = pl.ds(pl.multiple_of((g * group + j) * HD, HD), HD)
                scores = lax.dot_general(
                    q_buf[s, :, cols],
                    keys,
                    (((1,), (1,)), ((), ())),
                    preferred_element_type=jnp.float32,
                ) / math.sqrt(HD)
                scores = jnp.where(causal, scores, -1e30)
                highest = jnp.max(scores, axis=-1, keepdims=True)
                expd = jnp.exp(scores - highest)
                att = (expd / jnp.sum(expd, axis=-1, keepdims=True)).astype(jnp.bfloat16)
                both += lax.dot_general(
                    att,
                    jnp.concatenate([att, t_buf[s, :, cols]], axis=1),
                    (((0,), (0,)), ((), ())),
                    preferred_element_type=jnp.float32,
                )
            mat[0, s, g] = both[:, :length].astype(jnp.bfloat16)
            base[0, s, g] = both[:, length:].astype(jnp.bfloat16)
            return carry

        lax.fori_loop(0, heads, one, 0)

    def send_products(s, cond, keep):
        return [
            send_if(cond, keep, buf.at[0, s], buf.at[1, s], mat_s.at[s, i], mat_r.at[s, i], partner)
            for i, buf in enumerate((mat, base))
        ]

    chunk = 32

    def over(start, size, body):
        def step(i, carry):
            body(i * chunk)
            return carry

        lax.fori_loop(0, size // chunk, step, 0)

    order = [(a, b, dc) for a, b in quads for dc in (1, 0)]
    send_inputs(0, order[:4])
    loads[0].wait()

    def cast_weights(r):
        wb[0, at(r, chunk), :] = w_buf[at(r, chunk), :].astype(jnp.bfloat16)

    over(0, rows, cast_weights)
    mid = rows // 2
    w_mine = at(y * mid, mid)
    w_cross = send_if(
        far, far_pending, wb.at[0, w_mine], wb.at[1, w_mine], w_s.at[0], w_r.at[0], partner
    )
    send_inputs(0, order[4:])
    for s in range(1, steps):
        send_inputs(s, order, near, near_pending)
    for i in (1, 2, 3):
        loads[i].wait()
    attention_of(0)
    products = [send_products(0, far, far_pending)]
    for s in range(1, steps):
        send_inputs(s, order, beside, far_pending)
    wait_if(far, w_cross)
    w_relay = send_if(
        far, far_pending, wb.at[1, w_mine], wb.at[1, w_mine], w_s.at[1], w_r.at[1], y_peer
    )
    for s in range(1, steps):
        attention_of(s)
        products.append(send_products(s, beside, far_pending))
    wait_if(far, w_relay)

    def weights(s, p):
        return wb[sel, :, wide[p]] if s == 0 else w_now[:, wide[p]]

    sides = ((half * quad, near, far, near_pending, far_pending),
             ((1 - half) * quad, far, near, far_pending, near_pending))
    slot = at(me_slot(core, low, x) * length, length)
    for s in range(steps):

        def scatter(start, taker, giver, keep, keep_giver):
            for a, b in quads:
                wait_input(s, start // length + ((low + a) % 2) * 2 + (x + b) % 2)
            pairs, reds = {}, {}
            for p in range(parts):
                for a in (1, 0):
                    first = ((low + a) % 2) * 2 * length
                    span = at(first, 2 * length)
                    part = jnp.dot(
                        feat[s, at(start + first, 2 * length)],
                        weights(s, p),
                        preferred_element_type=jnp.float32,
                    )
                    own_part[span, wide[p]] = part

                    @pl.when(giver)
                    def _():
                        pair_out[s, span, wide[p]] = part.astype(jnp.bfloat16)

                    pairs[a, p] = send_if(
                        giver,
                        keep_giver,
                        pair_out.at[s, span, wide[p]],
                        pair_in.at[s, span, wide[p]],
                        pair_s.at[s, a, p],
                        pair_r.at[s, a, p],
                        core_peer,
                    )
            for p in range(parts):
                for a in (1, 0):
                    span = at(((low + a) % 2) * 2 * length, 2 * length)
                    wait_if(taker, pairs[a, p])

                    @pl.when(taker)
                    def _():
                        red_out[s, span, wide[p]] = (
                            own_part[span, wide[p]]
                            + pair_in[s, span, wide[p]].astype(jnp.float32)
                        ).astype(jnp.bfloat16)

                    for b in (1, 0):
                        if a + b:
                            reds[a, b, p] = send_if(
                                taker,
                                keep,
                                red_out.at[s, at(offset(a, b), length), wide[p]],
                                red_in.at[s, a * 2 + b, :, wide[p]],
                                red_s.at[s, a * 2 + b, p],
                                red_r.at[s, a * 2 + b, p],
                                mate(a, b),
                            )
            return reds

        def reduce(reds, start, taker, giver, keep, keep_giver):
            gathers, passes = {}, {}
            for p in range(parts):
                for a, b in quads[:3]:
                    wait_if(taker, reds[a, b, p])

                @pl.when(taker)
                def _():
                    summed = red_out[s, at(offset(0, 0), length), wide[p]].astype(jnp.float32)
                    for a, b in quads[:3]:
                        summed = summed + red_in[s, a * 2 + b, :, wide[p]].astype(jnp.float32)
                    values = (summed / math.sqrt(D)).astype(jnp.bfloat16)
                    for i in range(width // HD):
                        g = p * (width // HD) + i
                        part = values[:, i * HD : (i + 1) * HD]
                        vg = jnp.dot(mat[sel, s, g], part, preferred_element_type=jnp.float32)
                        vg = (vg - base[sel, s, g].astype(jnp.float32)) / tok_rep
                        vgrad[s, slot, g * HD : (g + 1) * HD] = vg.astype(jnp.bfloat16)

                block = vgrad.at[s, slot, wide[p]]
                for a, b in quads[:3]:
                    i = a * 2 + b
                    gathers[a, b, p] = send_if(
                        taker, keep, block, block, ag_s.at[s, i, p], ag_r.at[s, i, p], mate(a, b)
                    )
                passes[0, 0, p] = send_if(
                    taker, keep, block, block, fw_s.at[s, 0, p], fw_r.at[s, 0, p], core_peer
                )
            return gathers, passes

        def gather(copies, first, start, taker, giver, keep, keep_giver):
            gathers, passes = copies
            for p in range(parts):
                for a, b in quads[2::-1]:
                    wait_if(taker, gathers[a, b, p])
                    i = a * 2 + b
                    block = vgrad.at[s, at(start + offset(a, b), length), wide[p]]
                    passes[a, b, p] = send_if(
                        taker, keep, block, block, fw_s.at[s, i, p], fw_r.at[s, i, p], core_peer
                    )
            for p in range(parts):
                for a, b in quads[::-1]:
                    wait_if(giver, passes[a, b, p])
                term = lax.dot_general(
                    feat[s, at(start, quad)],
                    vgrad[s, at(start, quad), wide[p]],
                    (((0,), (0,)), ((), ())),
                    preferred_element_type=jnp.float32,
                )
                if first:
                    grad[s, :, wide[p]] = term
                else:
                    grad[s, :, wide[p]] += term

        near_reds = scatter(*sides[0])
        near_copies = reduce(near_reds, *sides[0])
        far_reds = scatter(*sides[1])
        gather(near_copies, True, *sides[0])
        for copy in products[s]:
            wait_if(far, copy)
        far_copies = reduce(far_reds, *sides[1])
        for later in range(s + 1, min(s + 2, steps)):
            send_inputs(later, order, outer, [])
            send_products(later, outer, [])
        gather(far_copies, False, *sides[1])

        def adam(r, keep):
            c = at(r, chunk)
            one, two = 0.0, 0.0
            for i in range(s + 1):
                gradient = grad[i, c, :] / math.sqrt(D)
                one = beta_one * one + (1.0 - beta_one) * gradient
                two = beta_two * two + (1.0 - beta_two) * gradient * gradient
            fixed_one = one / (1.0 - beta_one ** (s + 1))
            fixed_two = two / (1.0 - beta_two ** (s + 1))
            update = fixed_one / (jnp.sqrt(fixed_two) + adam_floor)
            keep(c, update)

        if s + 1 < steps:

            def keep(c, update):
                before = wb[sel, c, :].astype(jnp.float32)
                first_update[c, :] = update
                w_now[c, :] = (before * shrink - inner_rate * update).astype(jnp.bfloat16)

            over(0, rows, lambda r: adam(r, keep))

    def moved(c, update):
        return inner_rate * (shrink * first_update[c, :] + update)

    pieces = 4
    size = mid // pieces
    crosses, sums, overs, shared, third, fourth = [], [], [], [], [], []
    for p in range(pieces):

        def out_piece(r):
            def put(c, update):
                sy_out[at(p * size + r, chunk), :] = moved(c, update).astype(jnp.bfloat16)

            adam((1 - y) * mid + p * size + r, put)

        over(0, size, out_piece)
        piece = at(p * size, size)
        crosses.append(
            send(sy_out.at[piece], sy_in.at[piece], fin_s.at[0, p], fin_r.at[0, p], y_peer)
        )

    def own_rows(r):
        def put(c, update):
            s_own[at(r, chunk), :] = moved(c, update)

        adam(y * mid + r, put)

    over(0, mid, own_rows)
    for p in range(pieces):
        piece = at(p * size, size)
        crosses[p].wait_recv()

        def join(r):
            c = at(p * size + r, chunk)
            halves[2 * sel, c, :] = (s_own[c, :] + sy_in[c, :].astype(jnp.float32)).astype(
                jnp.bfloat16
            )

        over(0, size, join)
        overs.append(
            send_if(
                far,
                far_pending,
                halves.at[2, piece],
                halves.at[1, piece],
                fin_s.at[2, p],
                fin_r.at[2, p],
                partner,
            )
        )
        sums.append(
            send_if(
                near,
                near_pending,
                halves.at[0, piece],
                halves.at[0, piece],
                fin_s.at[1, p],
                fin_r.at[1, p],
                core_peer,
            )
        )
    y_cross = device(half, low, x, 1 - y, 1 - core)

    def copy_out(start, src):
        def one(r):
            mean_ref[at(start + r, chunk), :] = src(r)

        over(0, size, one)

    for p in range(pieces):
        piece = at(p * size, size)
        wait_if(far, sums[p])
        wait_if(far, overs[p])

        @pl.when(far)
        def _():
            def one(r):
                c = at(p * size + r, chunk)
                tot_mine[c, :] = (
                    halves[0, c, :].astype(jnp.float32) + halves[1, c, :].astype(jnp.float32)
                ).astype(jnp.bfloat16)

            over(0, size, one)

        mine_p, other_p = tot_mine.at[piece], tot_other.at[piece]
        third.append(
            send_if(far, far_pending, mine_p, other_p, fin_s.at[3, p], fin_r.at[3, p], y_peer)
        )
        fourth.append(
            send_if(far, far_pending, mine_p, other_p, fin_s.at[4, p], fin_r.at[4, p], y_cross)
        )
        shared.append(
            send_if(far, far_pending, mine_p, mine_p, fin_s.at[5, p], fin_r.at[5, p], core_peer)
        )
    for p in range(pieces):
        wait_if(near, shared[p])
        copy_out(y * mid + p * size, lambda r: tot_mine[at(p * size + r, chunk), :])
    for p in range(pieces):
        wait_if(far, third[p])
        wait_if(near, fourth[p])
        copy_out((1 - y) * mid + p * size, lambda r: tot_other[at(p * size + r, chunk), :])
    for copy in pending:
        copy.wait_send()

    @pl.when(far)
    def _():
        for copy in far_pending:
            copy.wait_send()

    @pl.when(near)
    def _():
        for copy in near_pending:
            copy.wait_send()


def me_slot(core, low, x):
    return (core * 2 + low) * 2 + x


def shards(layer_input, queries, keys, targets, value_weight, outer_momentum):
    n = lax.axis_size("fsdp")
    replicas = lax.axis_size("replica")
    rows, columns = value_weight.shape
    steps, length, _ = layer_input.shape
    if rows % 512 or columns % (2 * HD) or n != 8 or replicas != 4 or length % 128 or steps != 2:
        return plain_shards(layer_input, queries, keys, targets, value_weight, outer_momentum)
    heads = columns // HD
    bf, f32 = jnp.bfloat16, jnp.float32
    dma = pltpu.SemaphoreType.DMA
    out = jax.ShapeDtypeStruct((rows, columns), bf)
    total_update = pl.pallas_call(
        round_kernel,
        out_shape=out,
        in_specs=[pl.BlockSpec(memory_space=pl.ANY)] * 5,
        out_specs=pl.BlockSpec(memory_space=pltpu.VMEM),
        scratch_shapes=[
            pltpu.VMEM((steps, n * length, rows), bf),
            pltpu.VMEM(queries.shape, bf),
            pltpu.VMEM(keys.shape, bf),
            pltpu.VMEM(targets.shape, bf),
            pltpu.VMEM((rows, columns), f32),
            pltpu.VMEM((2, rows, columns), bf),
            pltpu.VMEM((rows, columns), bf),
            pltpu.VMEM((4 * length, columns), f32),
            pltpu.VMEM((2, steps, heads, length, length), bf),
            pltpu.VMEM((2, steps, heads, length, HD), bf),
            pltpu.VMEM((steps, 4 * length, columns), bf),
            pltpu.VMEM((steps, 4 * length, columns), bf),
            pltpu.VMEM((steps, 4 * length, columns), bf),
            pltpu.VMEM((steps, 4, length, columns), bf),
            pltpu.VMEM((steps, n * length, columns), bf),
            pltpu.VMEM((steps, rows, columns), f32),
            pltpu.VMEM((rows, columns), f32),
            pltpu.VMEM((rows // 2, columns), bf),
            pltpu.VMEM((rows // 2, columns), bf),
            pltpu.VMEM((rows // 2, columns), f32),
            pltpu.VMEM((3, rows // 2, columns), bf),
            pltpu.VMEM((rows // 2, columns), bf),
            pltpu.VMEM((rows // 2, columns), bf),
            dma((steps, n)),
            dma((steps, n)),
            dma((2,)),
            dma((2,)),
            dma((steps, 2)),
            dma((steps, 2)),
            dma((steps, 2, 2)),
            dma((steps, 2, 2)),
            dma((steps, 4, 2)),
            dma((steps, 4, 2)),
            dma((steps, 4, 2)),
            dma((steps, 4, 2)),
            dma((steps, 4, 2)),
            dma((steps, 4, 2)),
            dma((6, 4)),
            dma((6, 4)),
            dma((4,)),
        ],
        compiler_params=pltpu.CompilerParams(collective_id=0, has_side_effects=True),
    )(layer_input, queries, keys, targets, value_weight)
    kept = (1.0 - inner_rate * decay_rate) ** steps
    mean_delta = (1.0 - kept) * value_weight + total_update.astype(f32) / replicas
    new_momentum = outer_mu * outer_momentum + mean_delta
    new_weight = value_weight - outer_rate * (mean_delta + outer_mu * new_momentum)
    return (new_weight, new_momentum)


def solution(mesh):
    in_specs = (
        P(None, ("replica", "fsdp"), None),
        P(None, ("replica", "fsdp"), None),
        P(None, ("replica", "fsdp"), None),
        P(None, ("replica", "fsdp"), None),
        P("fsdp", None),
        P("fsdp", None),
    )
    out_specs = (P("fsdp", None), P("fsdp", None))
    return jax.shard_map(shards, mesh=mesh, in_specs=in_specs, out_specs=out_specs, check_vma=False)
```

```python
import math

import jax
import jax.numpy as jnp
from jax import lax
from jax.experimental import pallas as pl
from jax.experimental.pallas import tpu as pltpu
from jax.sharding import PartitionSpec as P

D = 4096
QH = 32
KVH = 4
HD = 128


beta_one = 0.9
beta_two = 0.95
inner_rate = 0.05
decay_rate = 0.1
outer_rate = 0.7
outer_mu = 0.9


def plain_shards(layer_input, queries, keys, targets, value_weight, outer_momentum):
    inner_steps = layer_input.shape[0]
    length = layer_input.shape[1]
    columns = value_weight.shape[1]
    fsdp_count = lax.axis_size("fsdp")
    replicas = lax.axis_size("replica")
    tok_rep = length * fsdp_count
    group_size = QH // KVH
    adam_floor = math.sqrt(group_size / (tok_rep * D))
    by_features = lax.all_to_all(layer_input, "fsdp", split_axis=2, concat_axis=1, tiled=True)
    causal = jnp.arange(length)[:, None] >= jnp.arange(length)[None, :]
    weights_now = value_weight
    moment_one = jnp.zeros_like(value_weight)
    moment_two = jnp.zeros_like(value_weight)
    for step_index in range(inner_steps):
        inputs = layer_input[step_index]
        shard_bf = weights_now.astype(jnp.bfloat16)
        product = jnp.dot(
            inputs,
            lax.all_gather(shard_bf, "fsdp", axis=0, tiled=True),
            preferred_element_type=jnp.float32,
        )
        values = (product / math.sqrt(D)).astype(jnp.bfloat16)
        query_heads = queries[step_index].reshape(length, KVH, group_size, HD)
        key_heads = keys[step_index].reshape(length, KVH, HD)
        scores = jnp.einsum(
            "qgjd,kgd->gjqk", query_heads, key_heads, preferred_element_type=jnp.float32
        ) / math.sqrt(HD)
        scores = jnp.where(causal, scores, -1e30)
        highest = jnp.max(scores, axis=-1, keepdims=True)
        expd = jnp.exp(scores - highest)
        attention = (expd / jnp.sum(expd, axis=-1, keepdims=True)).astype(jnp.bfloat16)
        attended = jnp.einsum(
            "gjqk,kgd->qgjd",
            attention,
            values.reshape(length, KVH, HD),
            preferred_element_type=jnp.float32,
        ).reshape(length, QH * HD)
        out_grad = ((attended - targets[step_index].astype(jnp.float32)) / tok_rep).astype(
            jnp.bfloat16
        )
        value_grad = (
            jnp.einsum(
                "gjqk,qgjd->kgd",
                attention,
                out_grad.reshape(length, KVH, group_size, HD),
                preferred_element_type=jnp.float32,
            )
            .reshape(length, columns)
            .astype(jnp.bfloat16)
        )
        step_features = by_features[step_index]
        gradient = lax.dot_general(
            step_features,
            lax.all_gather(value_grad, "fsdp", axis=0, tiled=True),
            (((0,), (0,)), ((), ())),
            preferred_element_type=jnp.float32,
        ) / math.sqrt(D)
        moment_one = beta_one * moment_one + (1.0 - beta_one) * gradient
        moment_two = beta_two * moment_two + (1.0 - beta_two) * gradient * gradient
        corrected_one = moment_one / (1.0 - beta_one ** (step_index + 1))
        corrected_two = moment_two / (1.0 - beta_two ** (step_index + 1))
        weights_now = weights_now - inner_rate * (
            corrected_one / (jnp.sqrt(corrected_two) + adam_floor) + decay_rate * weights_now
        )
    total_delta = lax.psum(value_weight - weights_now, "replica")
    mean_delta = total_delta / replicas
    new_momentum = outer_mu * outer_momentum + mean_delta
    new_weight = value_weight - outer_rate * (mean_delta + outer_mu * new_momentum)
    return (new_weight, new_momentum)


MESH = pl.DeviceIdType.MESH


def round_kernel(
    x_ref,
    q_ref,
    k_ref,
    t_ref,
    w_ref,
    mean_ref,
    feat,
    q_buf,
    k_buf,
    t_buf,
    w_buf,
    wb,
    w_now,
    own_part,
    mat,
    base,
    pair_out,
    pair_in,
    red_out,
    red_in,
    vgrad,
    grad,
    first_update,
    sy_out,
    sy_in,
    s_own,
    halves,
    tot_mine,
    tot_other,
    in_s,
    in_r,
    w_s,
    w_r,
    mat_s,
    mat_r,
    pair_s,
    pair_r,
    red_s,
    red_r,
    ag_s,
    ag_r,
    fw_s,
    fw_r,
    fin_s,
    fin_r,
    load_s,
):
    steps, length, _ = x_ref.shape
    rows, columns = w_ref.shape
    parts = 2
    width = columns // parts
    wide = [slice(p * width, (p + 1) * width) for p in range(parts)]
    heads = columns // HD
    group = QH // KVH
    quad = 4 * length
    tok_rep = 2 * quad
    adam_floor = math.sqrt(group / (tok_rep * D))
    shrink = 1.0 - inner_rate * decay_rate
    me = lax.axis_index("fsdp")
    rep = lax.axis_index("replica")
    x = me % 2
    low = (me // 2) % 2
    half = me // 4
    y = rep // 2
    core = rep % 2
    sel = (half + core) % 2
    far = sel == 1
    near = sel == 0
    beside = jnp.logical_and(far, low != half)
    outer = jnp.logical_and(far, low == half)

    def device(h, l, xx, yy, cc):
        return {"replica": yy * 2 + cc, "fsdp": (h * 2 + l) * 2 + xx}

    core_peer = device(half, low, x, y, 1 - core)
    y_peer = device(half, low, x, 1 - y, core)
    partner = device(core, low, x, y, half)

    def mate(a, b):
        return device(half, (low + a) % 2, (x + b) % 2, y, core)

    def offset(a, b):
        return (((low + a) % 2) * 2 + (x + b) % 2) * length

    quads = [(1, 1), (0, 1), (1, 0), (0, 0)]

    def at(start, size):
        return pl.ds(pl.multiple_of(start, 32), size)

    loads = {}

    def load(i, src, dst):
        loads[i] = pltpu.make_async_copy(src, dst, load_s.at[i])
        loads[i].start()

    barrier = pltpu.get_barrier_semaphore()
    count = 0
    for dh in range(2):
        for dl in range(2):
            for dx in range(2):
                for dc in range(2):
                    if dh + dl + dx + dc:
                        peer = device(
                            (half + dh) % 2, (low + dl) % 2, (x + dx) % 2, y, (core + dc) % 2
                        )
                        pl.semaphore_signal(barrier, inc=1, device_id=peer, device_id_type=MESH)
                        count += 1
    for dc in range(2):
        peer = device(half, low, x, 1 - y, (core + dc) % 2)
        pl.semaphore_signal(barrier, inc=1, device_id=peer, device_id_type=MESH)
    load(0, w_ref, w_buf)
    load(1, q_ref, q_buf)
    load(2, k_ref, k_buf)
    load(3, t_ref, t_buf)
    pl.semaphore_wait(barrier, count + 2)

    pending, far_pending, near_pending = [], [], []

    def remote(src, dst, ssem, rsem, peer):
        return pltpu.make_async_remote_copy(
            src_ref=src,
            dst_ref=dst,
            send_sem=ssem,
            recv_sem=rsem,
            device_id=peer,
            device_id_type=MESH,
        )

    def send(*args):
        copy = remote(*args)
        copy.start()
        pending.append(copy)
        return copy

    def send_if(cond, keep, *args):
        copy = remote(*args)

        @pl.when(cond)
        def _():
            copy.start()

        keep.append(copy)
        return copy

    def wait_if(cond, copy):
        @pl.when(cond)
        def _():
            copy.wait_recv()

    def send_inputs(s, picks, cond=None, keep=None):
        for a, b, dc in picks:
            l2, x2, c2 = (low + a) % 2, (x + b) % 2, (core + dc) % 2
            i = a * 4 + b * 2 + dc
            src = x_ref.at[
                s, :, pl.ds(pl.multiple_of(((c2 * 2 + l2) * 2 + x2) * rows, 128), rows)
            ]
            dst = feat.at[s, at(me * length, length)]
            args = (src, dst, in_s.at[s, i], in_r.at[s, me], device(core, l2, x2, y, c2))
            if i and cond is None:
                send(*args)
            elif i:
                send_if(cond, keep, *args)
            else:
                if cond is not near:
                    send_if(far if cond is None else cond, far_pending if cond is None else keep, *args)
                if cond is None or cond is near:

                    @pl.when(near)
                    def _():
                        pltpu.make_async_copy(src, dst, in_r.at[s, me]).start()

    def wait_input(s, j):
        slot = feat.at[s, at(j * length, length)]
        remote(slot, slot, in_s.at[s, 0], in_r.at[s, j], core_peer).wait_recv()

    causal = lax.broadcasted_iota(jnp.int32, (length, length), 0) >= lax.broadcasted_iota(
        jnp.int32, (length, length), 1
    )

    def attention_of(s):
        def one(g, carry):
            keys = k_buf[s, :, pl.ds(pl.multiple_of(g * HD, HD), HD)]
            both = jnp.zeros((length, length + HD), jnp.float32)
            for j in range(group):
                cols = pl.ds(pl.multiple_of((g * group + j) * HD, HD), HD)
                scores = lax.dot_general(
                    q_buf[s, :, cols],
                    keys,
                    (((1,), (1,)), ((), ())),
                    preferred_element_type=jnp.float32,
                ) / math.sqrt(HD)
                scores = jnp.where(causal, scores, -1e30)
                highest = jnp.max(scores, axis=-1, keepdims=True)
                expd = jnp.exp(scores - highest)
                att = (expd / jnp.sum(expd, axis=-1, keepdims=True)).astype(jnp.bfloat16)
                both += lax.dot_general(
                    att,
                    jnp.concatenate([att, t_buf[s, :, cols]], axis=1),
                    (((0,), (0,)), ((), ())),
                    preferred_element_type=jnp.float32,
                )
            mat[0, s, g] = both[:, :length].astype(jnp.bfloat16)
            base[0, s, g] = both[:, length:].astype(jnp.bfloat16)
            return carry

        lax.fori_loop(0, heads, one, 0)

    def send_products(s, cond, keep):
        return [
            send_if(cond, keep, buf.at[0, s], buf.at[1, s], mat_s.at[s, i], mat_r.at[s, i], partner)
            for i, buf in enumerate((mat, base))
        ]

    chunk = 32

    def over(start, size, body):
        def step(i, carry):
            body(i * chunk)
            return carry

        lax.fori_loop(0, size // chunk, step, 0)

    order = [(a, b, dc) for a, b in quads for dc in (1, 0)]
    send_inputs(0, order[:4])
    loads[0].wait()

    def cast_weights(r):
        wb[0, at(r, chunk), :] = w_buf[at(r, chunk), :].astype(jnp.bfloat16)

    over(0, rows, cast_weights)
    mid = rows // 2
    w_mine = at(y * mid, mid)
    w_cross = send_if(
        far, far_pending, wb.at[0, w_mine], wb.at[1, w_mine], w_s.at[0], w_r.at[0], partner
    )
    send_inputs(0, order[4:])
    for s in range(1, steps):
        send_inputs(s, order, near, near_pending)
    for i in (1, 2, 3):
        loads[i].wait()
    attention_of(0)
    products = [send_products(0, far, far_pending)]
    for s in range(1, steps):
        send_inputs(s, order, beside, far_pending)
    wait_if(far, w_cross)
    w_relay = send_if(
        far, far_pending, wb.at[1, w_mine], wb.at[1, w_mine], w_s.at[1], w_r.at[1], y_peer
    )
    for s in range(1, steps):
        attention_of(s)
    wait_if(far, w_relay)

    def weights(s, p):
        return wb[sel, :, wide[p]] if s == 0 else w_now[:, wide[p]]

    sides = ((half * quad, near, far, near_pending, far_pending),
             ((1 - half) * quad, far, near, far_pending, near_pending))
    slot = at(me_slot(core, low, x) * length, length)
    for s in range(steps):

        def scatter(start, taker, giver, keep, keep_giver):
            for a, b in quads:
                wait_input(s, start // length + ((low + a) % 2) * 2 + (x + b) % 2)
            pairs, reds = {}, {}
            for p in range(parts):
                for a in (1, 0):
                    first = ((low + a) % 2) * 2 * length
                    span = at(first, 2 * length)
                    part = jnp.dot(
                        feat[s, at(start + first, 2 * length)],
                        weights(s, p),
                        preferred_element_type=jnp.float32,
                    )
                    own_part[span, wide[p]] = part

                    @pl.when(giver)
                    def _():
                        pair_out[s, span, wide[p]] = part.astype(jnp.bfloat16)

                    pairs[a, p] = send_if(
                        giver,
                        keep_giver,
                        pair_out.at[s, span, wide[p]],
                        pair_in.at[s, span, wide[p]],
                        pair_s.at[s, a, p],
                        pair_r.at[s, a, p],
                        core_peer,
                    )
            for p in range(parts):
                for a in (1, 0):
                    span = at(((low + a) % 2) * 2 * length, 2 * length)
                    wait_if(taker, pairs[a, p])

                    @pl.when(taker)
                    def _():
                        red_out[s, span, wide[p]] = (
                            own_part[span, wide[p]]
                            + pair_in[s, span, wide[p]].astype(jnp.float32)
                        ).astype(jnp.bfloat16)

                    for b in (1, 0):
                        if a + b:
                            reds[a, b, p] = send_if(
                                taker,
                                keep,
                                red_out.at[s, at(offset(a, b), length), wide[p]],
                                red_in.at[s, a * 2 + b, :, wide[p]],
                                red_s.at[s, a * 2 + b, p],
                                red_r.at[s, a * 2 + b, p],
                                mate(a, b),
                            )
            return reds

        def reduce(reds, start, taker, giver, keep, keep_giver):
            gathers, passes = {}, {}
            for p in range(parts):
                for a, b in quads[:3]:
                    wait_if(taker, reds[a, b, p])

                @pl.when(taker)
                def _():
                    summed = red_out[s, at(offset(0, 0), length), wide[p]].astype(jnp.float32)
                    for a, b in quads[:3]:
                        summed = summed + red_in[s, a * 2 + b, :, wide[p]].astype(jnp.float32)
                    values = (summed / math.sqrt(D)).astype(jnp.bfloat16)
                    for i in range(width // HD):
                        g = p * (width // HD) + i
                        part = values[:, i * HD : (i + 1) * HD]
                        vg = jnp.dot(mat[sel, s, g], part, preferred_element_type=jnp.float32)
                        vg = (vg - base[sel, s, g].astype(jnp.float32)) / tok_rep
                        vgrad[s, slot, g * HD : (g + 1) * HD] = vg.astype(jnp.bfloat16)

                block = vgrad.at[s, slot, wide[p]]
                for a, b in quads[:3]:
                    i = a * 2 + b
                    gathers[a, b, p] = send_if(
                        taker, keep, block, block, ag_s.at[s, i, p], ag_r.at[s, i, p], mate(a, b)
                    )
                passes[0, 0, p] = send_if(
                    taker, keep, block, block, fw_s.at[s, 0, p], fw_r.at[s, 0, p], core_peer
                )
            return gathers, passes

        def forward(copies, p, start, taker, giver, keep, keep_giver):
            gathers, passes = copies
            for a, b in quads[2::-1]:
                wait_if(taker, gathers[a, b, p])
                i = a * 2 + b
                block = vgrad.at[s, at(start + offset(a, b), length), wide[p]]
                passes[a, b, p] = send_if(
                    taker, keep, block, block, fw_s.at[s, i, p], fw_r.at[s, i, p], core_peer
                )

        def add_quad(copies, first, p, start, taker, giver, keep, keep_giver):
            for a, b in quads[::-1]:
                wait_if(giver, copies[1][a, b, p])
            term = lax.dot_general(
                feat[s, at(start, quad)],
                vgrad[s, at(start, quad), wide[p]],
                (((0,), (0,)), ((), ())),
                preferred_element_type=jnp.float32,
            )
            if first:
                grad[s, :, wide[p]] = term
            else:
                grad[s, :, wide[p]] += term

        near_reds = scatter(*sides[0])
        if s:
            products.append(send_products(s, far, far_pending))
        near_copies = reduce(near_reds, *sides[0])
        far_reds = scatter(*sides[1])
        if s + 1 < steps:
            send_inputs(s + 1, order[:2], outer, [])
        for p in range(parts):
            forward(near_copies, p, *sides[0])
        for p in range(parts):
            add_quad(near_copies, True, p, *sides[0])
        for copy in products[s]:
            wait_if(far, copy)
        far_copies = reduce(far_reds, *sides[1])
        if s + 1 < steps:
            send_inputs(s + 1, order[2:], outer, [])
            for p in range(parts):
                forward(far_copies, p, *sides[1])
            for p in range(parts):
                add_quad(far_copies, False, p, *sides[1])

        def adam(r, cols, keep):
            c = at(r, chunk)
            one, two = 0.0, 0.0
            for i in range(s + 1):
                gradient = grad[i, c, cols] / math.sqrt(D)
                one = beta_one * one + (1.0 - beta_one) * gradient
                two = beta_two * two + (1.0 - beta_two) * gradient * gradient
            fixed_one = one / (1.0 - beta_one ** (s + 1))
            fixed_two = two / (1.0 - beta_two ** (s + 1))
            keep(c, fixed_one / (jnp.sqrt(fixed_two) + adam_floor))

        if s + 1 < steps:

            def keep(c, update):
                before = wb[sel, c, :].astype(jnp.float32)
                first_update[c, :] = update
                w_now[c, :] = (before * shrink - inner_rate * update).astype(jnp.bfloat16)

            over(0, rows, lambda r: adam(r, slice(None), keep))

    pieces = 2
    size = mid // pieces
    crosses, sums, overs, shared, third, fourth = {}, {}, {}, {}, {}, {}
    cells = [(p, i) for p in range(parts) for i in range(pieces)]

    def moved(c, cols, update):
        return inner_rate * (shrink * first_update[c, cols] + update)

    def cell(ref, p, i):
        return ref.at[at(i * size, size), wide[p]]

    for p in range(parts):
        forward(far_copies, p, *sides[1])
        add_quad(far_copies, False, p, *sides[1])
        for i in range(pieces):

            def out_rows(r):
                def put(c, update):
                    sy_out[at(i * size + r, chunk), wide[p]] = moved(c, wide[p], update).astype(
                        jnp.bfloat16
                    )

                adam((1 - y) * mid + i * size + r, wide[p], put)

            over(0, size, out_rows)
            k = p * pieces + i
            crosses[p, i] = send(
                cell(sy_out, p, i), cell(sy_in, p, i), fin_s.at[0, k], fin_r.at[0, k], y_peer
            )
    for p in range(parts):

        def own_rows(r):
            def put(c, update):
                s_own[at(r, chunk), wide[p]] = moved(c, wide[p], update)

            adam(y * mid + r, wide[p], put)

        over(0, mid, own_rows)
    for p, i in cells:
        k = p * pieces + i
        crosses[p, i].wait_recv()

        def join(r):
            c = at(i * size + r, chunk)
            halves[2 * sel, c, wide[p]] = (
                s_own[c, wide[p]] + sy_in[c, wide[p]].astype(jnp.float32)
            ).astype(jnp.bfloat16)

        over(0, size, join)
        overs[p, i] = send_if(
            far,
            far_pending,
            cell(halves.at[2], p, i),
            cell(halves.at[1], p, i),
            fin_s.at[2, k],
            fin_r.at[2, k],
            partner,
        )
        sums[p, i] = send_if(
            near,
            near_pending,
            cell(halves.at[0], p, i),
            cell(halves.at[0], p, i),
            fin_s.at[1, k],
            fin_r.at[1, k],
            core_peer,
        )
    y_cross = device(half, low, x, 1 - y, 1 - core)

    for p, i in cells:
        k = p * pieces + i
        wait_if(far, sums[p, i])
        wait_if(far, overs[p, i])

        @pl.when(far)
        def _():
            def one(r):
                c = at(i * size + r, chunk)
                tot_mine[c, wide[p]] = (
                    halves[0, c, wide[p]].astype(jnp.float32)
                    + halves[1, c, wide[p]].astype(jnp.float32)
                ).astype(jnp.bfloat16)

            over(0, size, one)

        mine_p, other_p = cell(tot_mine, p, i), cell(tot_other, p, i)
        third[p, i] = send_if(
            far, far_pending, mine_p, other_p, fin_s.at[3, k], fin_r.at[3, k], y_peer
        )
        fourth[p, i] = send_if(
            far, far_pending, mine_p, other_p, fin_s.at[4, k], fin_r.at[4, k], y_cross
        )
        shared[p, i] = send_if(
            far, far_pending, mine_p, mine_p, fin_s.at[5, k], fin_r.at[5, k], core_peer
        )

    def copy_out(start, p, i, src):
        def one(r):
            mean_ref[at(start + i * size + r, chunk), wide[p]] = src[
                at(i * size + r, chunk), wide[p]
            ]

        over(0, size, one)

    for p, i in cells:
        wait_if(near, shared[p, i])
        copy_out(y * mid, p, i, tot_mine)
    for p, i in cells:
        wait_if(far, third[p, i])
        wait_if(near, fourth[p, i])
        copy_out((1 - y) * mid, p, i, tot_other)
    for copy in pending:
        copy.wait_send()

    @pl.when(far)
    def _():
        for copy in far_pending:
            copy.wait_send()

    @pl.when(near)
    def _():
        for copy in near_pending:
            copy.wait_send()


def me_slot(core, low, x):
    return (core * 2 + low) * 2 + x


def shards(layer_input, queries, keys, targets, value_weight, outer_momentum):
    n = lax.axis_size("fsdp")
    replicas = lax.axis_size("replica")
    rows, columns = value_weight.shape
    steps, length, _ = layer_input.shape
    if rows % 512 or columns % (2 * HD) or n != 8 or replicas != 4 or length % 128 or steps != 2:
        return plain_shards(layer_input, queries, keys, targets, value_weight, outer_momentum)
    heads = columns // HD
    bf, f32 = jnp.bfloat16, jnp.float32
    dma = pltpu.SemaphoreType.DMA
    out = jax.ShapeDtypeStruct((rows, columns), bf)
    total_update = pl.pallas_call(
        round_kernel,
        out_shape=out,
        in_specs=[pl.BlockSpec(memory_space=pl.ANY)] * 5,
        out_specs=pl.BlockSpec(memory_space=pltpu.VMEM),
        scratch_shapes=[
            pltpu.VMEM((steps, n * length, rows), bf),
            pltpu.VMEM(queries.shape, bf),
            pltpu.VMEM(keys.shape, bf),
            pltpu.VMEM(targets.shape, bf),
            pltpu.VMEM((rows, columns), f32),
            pltpu.VMEM((2, rows, columns), bf),
            pltpu.VMEM((rows, columns), bf),
            pltpu.VMEM((4 * length, columns), f32),
            pltpu.VMEM((2, steps, heads, length, length), bf),
            pltpu.VMEM((2, steps, heads, length, HD), bf),
            pltpu.VMEM((steps, 4 * length, columns), bf),
            pltpu.VMEM((steps, 4 * length, columns), bf),
            pltpu.VMEM((steps, 4 * length, columns), bf),
            pltpu.VMEM((steps, 4, length, columns), bf),
            pltpu.VMEM((steps, n * length, columns), bf),
            pltpu.VMEM((steps, rows, columns), f32),
            pltpu.VMEM((rows, columns), f32),
            pltpu.VMEM((rows // 2, columns), bf),
            pltpu.VMEM((rows // 2, columns), bf),
            pltpu.VMEM((rows // 2, columns), f32),
            pltpu.VMEM((3, rows // 2, columns), bf),
            pltpu.VMEM((rows // 2, columns), bf),
            pltpu.VMEM((rows // 2, columns), bf),
            dma((steps, n)),
            dma((steps, n)),
            dma((2,)),
            dma((2,)),
            dma((steps, 2)),
            dma((steps, 2)),
            dma((steps, 2, 2)),
            dma((steps, 2, 2)),
            dma((steps, 4, 2)),
            dma((steps, 4, 2)),
            dma((steps, 4, 2)),
            dma((steps, 4, 2)),
            dma((steps, 4, 2)),
            dma((steps, 4, 2)),
            dma((6, 4)),
            dma((6, 4)),
            dma((4,)),
        ],
        compiler_params=pltpu.CompilerParams(collective_id=0, has_side_effects=True),
    )(layer_input, queries, keys, targets, value_weight)
    kept = (1.0 - inner_rate * decay_rate) ** steps
    mean_delta = (1.0 - kept) * value_weight + total_update.astype(f32) / replicas
    new_momentum = outer_mu * outer_momentum + mean_delta
    new_weight = value_weight - outer_rate * (mean_delta + outer_mu * new_momentum)
    return (new_weight, new_momentum)


def solution(mesh):
    in_specs = (
        P(None, ("replica", "fsdp"), None),
        P(None, ("replica", "fsdp"), None),
        P(None, ("replica", "fsdp"), None),
        P(None, ("replica", "fsdp"), None),
        P("fsdp", None),
        P("fsdp", None),
    )
    out_specs = (P("fsdp", None), P("fsdp", None))
    return jax.shard_map(shards, mesh=mesh, in_specs=in_specs, out_specs=out_specs, check_vma=False)
```

```python
import math

import jax
import jax.numpy as jnp
from jax import lax
from jax.experimental import pallas as pl
from jax.experimental.pallas import tpu as pltpu
from jax.sharding import PartitionSpec as P

D = 4096
QH = 32
KVH = 4
HD = 128


beta_one = 0.9
beta_two = 0.95
inner_rate = 0.05
decay_rate = 0.1
outer_rate = 0.7
outer_mu = 0.9


def plain_shards(layer_input, queries, keys, targets, value_weight, outer_momentum):
    inner_steps = layer_input.shape[0]
    length = layer_input.shape[1]
    columns = value_weight.shape[1]
    fsdp_count = lax.axis_size("fsdp")
    replicas = lax.axis_size("replica")
    tok_rep = length * fsdp_count
    group_size = QH // KVH
    adam_floor = math.sqrt(group_size / (tok_rep * D))
    by_features = lax.all_to_all(layer_input, "fsdp", split_axis=2, concat_axis=1, tiled=True)
    causal = jnp.arange(length)[:, None] >= jnp.arange(length)[None, :]
    weights_now = value_weight
    moment_one = jnp.zeros_like(value_weight)
    moment_two = jnp.zeros_like(value_weight)
    for step_index in range(inner_steps):
        inputs = layer_input[step_index]
        shard_bf = weights_now.astype(jnp.bfloat16)
        product = jnp.dot(
            inputs,
            lax.all_gather(shard_bf, "fsdp", axis=0, tiled=True),
            preferred_element_type=jnp.float32,
        )
        values = (product / math.sqrt(D)).astype(jnp.bfloat16)
        query_heads = queries[step_index].reshape(length, KVH, group_size, HD)
        key_heads = keys[step_index].reshape(length, KVH, HD)
        scores = jnp.einsum(
            "qgjd,kgd->gjqk", query_heads, key_heads, preferred_element_type=jnp.float32
        ) / math.sqrt(HD)
        scores = jnp.where(causal, scores, -1e30)
        highest = jnp.max(scores, axis=-1, keepdims=True)
        expd = jnp.exp(scores - highest)
        attention = (expd / jnp.sum(expd, axis=-1, keepdims=True)).astype(jnp.bfloat16)
        attended = jnp.einsum(
            "gjqk,kgd->qgjd",
            attention,
            values.reshape(length, KVH, HD),
            preferred_element_type=jnp.float32,
        ).reshape(length, QH * HD)
        out_grad = ((attended - targets[step_index].astype(jnp.float32)) / tok_rep).astype(
            jnp.bfloat16
        )
        value_grad = (
            jnp.einsum(
                "gjqk,qgjd->kgd",
                attention,
                out_grad.reshape(length, KVH, group_size, HD),
                preferred_element_type=jnp.float32,
            )
            .reshape(length, columns)
            .astype(jnp.bfloat16)
        )
        step_features = by_features[step_index]
        gradient = lax.dot_general(
            step_features,
            lax.all_gather(value_grad, "fsdp", axis=0, tiled=True),
            (((0,), (0,)), ((), ())),
            preferred_element_type=jnp.float32,
        ) / math.sqrt(D)
        moment_one = beta_one * moment_one + (1.0 - beta_one) * gradient
        moment_two = beta_two * moment_two + (1.0 - beta_two) * gradient * gradient
        corrected_one = moment_one / (1.0 - beta_one ** (step_index + 1))
        corrected_two = moment_two / (1.0 - beta_two ** (step_index + 1))
        weights_now = weights_now - inner_rate * (
            corrected_one / (jnp.sqrt(corrected_two) + adam_floor) + decay_rate * weights_now
        )
    total_delta = lax.psum(value_weight - weights_now, "replica")
    mean_delta = total_delta / replicas
    new_momentum = outer_mu * outer_momentum + mean_delta
    new_weight = value_weight - outer_rate * (mean_delta + outer_mu * new_momentum)
    return (new_weight, new_momentum)


MESH = pl.DeviceIdType.MESH


def round_kernel(
    x_ref,
    q_ref,
    k_ref,
    t_ref,
    w_ref,
    mean_ref,
    feat,
    q_buf,
    k_buf,
    t_buf,
    w_buf,
    wb,
    w_now,
    own_part,
    mat,
    base,
    pair_out,
    pair_in,
    red_out,
    red_in,
    vgrad,
    grad,
    first_update,
    sy_out,
    sy_in,
    s_own,
    halves,
    tot_mine,
    tot_other,
    in_s,
    in_r,
    w_s,
    w_r,
    mat_s,
    mat_r,
    pair_s,
    pair_r,
    red_s,
    red_r,
    ag_s,
    ag_r,
    fw_s,
    fw_r,
    fin_s,
    fin_r,
    load_s,
):
    steps, length, _ = x_ref.shape
    rows, columns = w_ref.shape
    parts = 2
    width = columns // parts
    wide = [slice(p * width, (p + 1) * width) for p in range(parts)]
    heads = columns // HD
    group = QH // KVH
    quad = 4 * length
    tok_rep = 2 * quad
    adam_floor = math.sqrt(group / (tok_rep * D))
    shrink = 1.0 - inner_rate * decay_rate
    me = lax.axis_index("fsdp")
    rep = lax.axis_index("replica")
    x = me % 2
    low = (me // 2) % 2
    half = me // 4
    y = rep // 2
    core = rep % 2
    sel = (half + core) % 2
    far = sel == 1
    near = sel == 0
    beside = jnp.logical_and(far, low != half)
    outer = jnp.logical_and(far, low == half)

    def device(h, l, xx, yy, cc):
        return {"replica": yy * 2 + cc, "fsdp": (h * 2 + l) * 2 + xx}

    core_peer = device(half, low, x, y, 1 - core)
    y_peer = device(half, low, x, 1 - y, core)
    partner = device(core, low, x, y, half)

    def mate(a, b):
        return device(half, (low + a) % 2, (x + b) % 2, y, core)

    def offset(a, b):
        return (((low + a) % 2) * 2 + (x + b) % 2) * length

    quads = [(1, 1), (0, 1), (1, 0), (0, 0)]

    def at(start, size):
        return pl.ds(pl.multiple_of(start, 32), size)

    loads = {}

    def load(i, src, dst):
        loads[i] = pltpu.make_async_copy(src, dst, load_s.at[i])
        loads[i].start()

    barrier = pltpu.get_barrier_semaphore()
    count = 0
    for dh in range(2):
        for dl in range(2):
            for dx in range(2):
                for dc in range(2):
                    if dh + dl + dx + dc:
                        peer = device(
                            (half + dh) % 2, (low + dl) % 2, (x + dx) % 2, y, (core + dc) % 2
                        )
                        pl.semaphore_signal(barrier, inc=1, device_id=peer, device_id_type=MESH)
                        count += 1
    for dc in range(2):
        peer = device(half, low, x, 1 - y, (core + dc) % 2)
        pl.semaphore_signal(barrier, inc=1, device_id=peer, device_id_type=MESH)
    load(0, w_ref, w_buf)
    load(1, q_ref, q_buf)
    load(2, k_ref, k_buf)
    load(3, t_ref, t_buf)
    pl.semaphore_wait(barrier, count + 2)

    pending, far_pending, near_pending = [], [], []

    def remote(src, dst, ssem, rsem, peer):
        return pltpu.make_async_remote_copy(
            src_ref=src,
            dst_ref=dst,
            send_sem=ssem,
            recv_sem=rsem,
            device_id=peer,
            device_id_type=MESH,
        )

    def send(*args):
        copy = remote(*args)
        copy.start()
        pending.append(copy)
        return copy

    def send_if(cond, keep, *args):
        copy = remote(*args)

        @pl.when(cond)
        def _():
            copy.start()

        keep.append(copy)
        return copy

    def wait_if(cond, copy):
        @pl.when(cond)
        def _():
            copy.wait_recv()

    def send_inputs(s, picks, cond=None, keep=None):
        for a, b, dc in picks:
            l2, x2, c2 = (low + a) % 2, (x + b) % 2, (core + dc) % 2
            i = a * 4 + b * 2 + dc
            src = x_ref.at[
                s, :, pl.ds(pl.multiple_of(((c2 * 2 + l2) * 2 + x2) * rows, 128), rows)
            ]
            dst = feat.at[s, at(me * length, length)]
            args = (src, dst, in_s.at[s, i], in_r.at[s, me], device(core, l2, x2, y, c2))
            if i and cond is None:
                send(*args)
            elif i:
                send_if(cond, keep, *args)
            else:
                if cond is not near:
                    send_if(far if cond is None else cond, far_pending if cond is None else keep, *args)
                if cond is None or cond is near:

                    @pl.when(near)
                    def _():
                        pltpu.make_async_copy(src, dst, in_r.at[s, me]).start()

    def wait_input(s, j):
        slot = feat.at[s, at(j * length, length)]
        remote(slot, slot, in_s.at[s, 0], in_r.at[s, j], core_peer).wait_recv()

    causal = lax.broadcasted_iota(jnp.int32, (length, length), 0) >= lax.broadcasted_iota(
        jnp.int32, (length, length), 1
    )

    def attention_of(s):
        def one(g, carry):
            keys = k_buf[s, :, pl.ds(pl.multiple_of(g * HD, HD), HD)]
            both = jnp.zeros((length, length + HD), jnp.float32)
            for j in range(group):
                cols = pl.ds(pl.multiple_of((g * group + j) * HD, HD), HD)
                scores = lax.dot_general(
                    q_buf[s, :, cols],
                    keys,
                    (((1,), (1,)), ((), ())),
                    preferred_element_type=jnp.float32,
                ) / math.sqrt(HD)
                scores = jnp.where(causal, scores, -1e30)
                highest = jnp.max(scores, axis=-1, keepdims=True)
                expd = jnp.exp(scores - highest)
                att = (expd / jnp.sum(expd, axis=-1, keepdims=True)).astype(jnp.bfloat16)
                both += lax.dot_general(
                    att,
                    jnp.concatenate([att, t_buf[s, :, cols]], axis=1),
                    (((0,), (0,)), ((), ())),
                    preferred_element_type=jnp.float32,
                )
            mat[0, s, g] = both[:, :length].astype(jnp.bfloat16)
            base[0, s, g] = both[:, length:].astype(jnp.bfloat16)
            return carry

        lax.fori_loop(0, heads, one, 0)

    def send_products(s, cond, keep):
        return [
            send_if(cond, keep, buf.at[0, s], buf.at[1, s], mat_s.at[s, i], mat_r.at[s, i], partner)
            for i, buf in enumerate((mat, base))
        ]

    chunk = 32

    def over(start, size, body):
        def step(i, carry):
            body(i * chunk)
            return carry

        lax.fori_loop(0, size // chunk, step, 0)

    order = [(a, b, dc) for a, b in quads for dc in (1, 0)]
    loads[0].wait()

    def cast_weights(r):
        wb[0, at(r, chunk), :] = w_buf[at(r, chunk), :].astype(jnp.bfloat16)

    over(0, rows, cast_weights)
    mid = rows // 2
    w_mine = at(y * mid, mid)
    w_cross = send_if(
        far, far_pending, wb.at[0, w_mine], wb.at[1, w_mine], w_s.at[0], w_r.at[0], partner
    )
    send_inputs(0, order)
    for s in range(1, steps):
        pass
    for i in (1, 2, 3):
        loads[i].wait()
    wait_if(far, w_cross)
    w_relay = send_if(
        far, far_pending, wb.at[1, w_mine], wb.at[1, w_mine], w_s.at[1], w_r.at[1], y_peer
    )
    attention_of(0)
    products = [send_products(0, far, far_pending)]
    for s in range(1, steps):
        send_inputs(s, order, beside, far_pending)
        send_inputs(s, order, near, near_pending)
    wait_if(far, w_relay)

    def weights(s, p):
        return wb[sel, :, wide[p]] if s == 0 else w_now[:, wide[p]]

    sides = ((half * quad, near, far, near_pending, far_pending),
             ((1 - half) * quad, far, near, far_pending, near_pending))
    slot = at(me_slot(core, low, x) * length, length)
    for s in range(steps):

        def scatter(start, taker, giver, keep, keep_giver):
            for a, b in quads:
                wait_input(s, start // length + ((low + a) % 2) * 2 + (x + b) % 2)
            pairs, reds = {}, {}
            for p in range(parts):
                for a in (1, 0):
                    first = ((low + a) % 2) * 2 * length
                    span = at(first, 2 * length)
                    part = jnp.dot(
                        feat[s, at(start + first, 2 * length)],
                        weights(s, p),
                        preferred_element_type=jnp.float32,
                    )
                    own_part[span, wide[p]] = part

                    @pl.when(giver)
                    def _():
                        pair_out[s, span, wide[p]] = part.astype(jnp.bfloat16)

                    pairs[a, p] = send_if(
                        giver,
                        keep_giver,
                        pair_out.at[s, span, wide[p]],
                        pair_in.at[s, span, wide[p]],
                        pair_s.at[s, a, p],
                        pair_r.at[s, a, p],
                        core_peer,
                    )
            for p in range(parts):
                for a in (1, 0):
                    span = at(((low + a) % 2) * 2 * length, 2 * length)
                    wait_if(taker, pairs[a, p])

                    @pl.when(taker)
                    def _():
                        red_out[s, span, wide[p]] = (
                            own_part[span, wide[p]]
                            + pair_in[s, span, wide[p]].astype(jnp.float32)
                        ).astype(jnp.bfloat16)

                    for b in (1, 0):
                        if a + b:
                            reds[a, b, p] = send_if(
                                taker,
                                keep,
                                red_out.at[s, at(offset(a, b), length), wide[p]],
                                red_in.at[s, a * 2 + b, :, wide[p]],
                                red_s.at[s, a * 2 + b, p],
                                red_r.at[s, a * 2 + b, p],
                                mate(a, b),
                            )
            return reds

        def reduce(reds, start, taker, giver, keep, keep_giver):
            gathers, passes = {}, {}
            for p in range(parts):
                for a, b in quads[:3]:
                    wait_if(taker, reds[a, b, p])

                @pl.when(taker)
                def _():
                    summed = red_out[s, at(offset(0, 0), length), wide[p]].astype(jnp.float32)
                    for a, b in quads[:3]:
                        summed = summed + red_in[s, a * 2 + b, :, wide[p]].astype(jnp.float32)
                    values = (summed / math.sqrt(D)).astype(jnp.bfloat16)
                    for i in range(width // HD):
                        g = p * (width // HD) + i
                        part = values[:, i * HD : (i + 1) * HD]
                        vg = jnp.dot(mat[sel, s, g], part, preferred_element_type=jnp.float32)
                        vg = (vg - base[sel, s, g].astype(jnp.float32)) / tok_rep
                        vgrad[s, slot, g * HD : (g + 1) * HD] = vg.astype(jnp.bfloat16)

                block = vgrad.at[s, slot, wide[p]]
                for a, b in quads[:3]:
                    i = a * 2 + b
                    gathers[a, b, p] = send_if(
                        taker, keep, block, block, ag_s.at[s, i, p], ag_r.at[s, i, p], mate(a, b)
                    )
                passes[0, 0, p] = send_if(
                    taker, keep, block, block, fw_s.at[s, 0, p], fw_r.at[s, 0, p], core_peer
                )
            return gathers, passes

        def forward(copies, p, start, taker, giver, keep, keep_giver):
            gathers, passes = copies
            for a, b in quads[2::-1]:
                wait_if(taker, gathers[a, b, p])
                i = a * 2 + b
                block = vgrad.at[s, at(start + offset(a, b), length), wide[p]]
                passes[a, b, p] = send_if(
                    taker, keep, block, block, fw_s.at[s, i, p], fw_r.at[s, i, p], core_peer
                )

        def add_quad(copies, first, p, start, taker, giver, keep, keep_giver):
            for a, b in quads[::-1]:
                wait_if(giver, copies[1][a, b, p])
            term = lax.dot_general(
                feat[s, at(start, quad)],
                vgrad[s, at(start, quad), wide[p]],
                (((0,), (0,)), ((), ())),
                preferred_element_type=jnp.float32,
            )
            if first:
                grad[s, :, wide[p]] = term
            else:
                grad[s, :, wide[p]] += term

        near_reds = scatter(*sides[0])
        if s:
            products.append(send_products(s, far, far_pending))
        near_copies = reduce(near_reds, *sides[0])
        if s + 1 < steps:
            attention_of(s + 1)
        far_reds = scatter(*sides[1])
        if s + 1 < steps:
            send_inputs(s + 1, order[:4], outer, [])
        for p in range(parts):
            forward(near_copies, p, *sides[0])
        for p in range(parts):
            add_quad(near_copies, True, p, *sides[0])
        for copy in products[s]:
            wait_if(far, copy)
        far_copies = reduce(far_reds, *sides[1])
        if s + 1 < steps:
            send_inputs(s + 1, order[4:], outer, [])
            for p in range(parts):
                forward(far_copies, p, *sides[1])
            for p in range(parts):
                add_quad(far_copies, False, p, *sides[1])

        def adam(r, cols, keep):
            c = at(r, chunk)
            one, two = 0.0, 0.0
            for i in range(s + 1):
                gradient = grad[i, c, cols] / math.sqrt(D)
                one = beta_one * one + (1.0 - beta_one) * gradient
                two = beta_two * two + (1.0 - beta_two) * gradient * gradient
            fixed_one = one / (1.0 - beta_one ** (s + 1))
            fixed_two = two / (1.0 - beta_two ** (s + 1))
            keep(c, fixed_one / (jnp.sqrt(fixed_two) + adam_floor))

        if s + 1 < steps:

            def keep(c, update):
                before = wb[sel, c, :].astype(jnp.float32)
                first_update[c, :] = update
                w_now[c, :] = (before * shrink - inner_rate * update).astype(jnp.bfloat16)

            over(0, rows, lambda r: adam(r, slice(None), keep))

    pieces = 2
    size = mid // pieces
    crosses, sums, overs, shared, third, fourth = {}, {}, {}, {}, {}, {}
    cells = [(p, i) for p in range(parts) for i in range(pieces)]

    def moved(c, cols, update):
        return inner_rate * (shrink * first_update[c, cols] + update)

    def cell(ref, p, i):
        return ref.at[at(i * size, size), wide[p]]

    for p in range(parts):
        forward(far_copies, p, *sides[1])
        add_quad(far_copies, False, p, *sides[1])
        for i in range(pieces):

            def out_rows(r):
                def put(c, update):
                    sy_out[at(i * size + r, chunk), wide[p]] = moved(c, wide[p], update).astype(
                        jnp.bfloat16
                    )

                adam((1 - y) * mid + i * size + r, wide[p], put)

            over(0, size, out_rows)
            k = p * pieces + i
            crosses[p, i] = send(
                cell(sy_out, p, i), cell(sy_in, p, i), fin_s.at[0, k], fin_r.at[0, k], y_peer
            )
    for p in range(parts):

        def own_rows(r):
            def put(c, update):
                s_own[at(r, chunk), wide[p]] = moved(c, wide[p], update)

            adam(y * mid + r, wide[p], put)

        over(0, mid, own_rows)
    for p, i in cells:
        k = p * pieces + i
        crosses[p, i].wait_recv()

        def join(r):
            c = at(i * size + r, chunk)
            halves[2 * sel, c, wide[p]] = (
                s_own[c, wide[p]] + sy_in[c, wide[p]].astype(jnp.float32)
            ).astype(jnp.bfloat16)

        over(0, size, join)
        overs[p, i] = send_if(
            far,
            far_pending,
            cell(halves.at[2], p, i),
            cell(halves.at[1], p, i),
            fin_s.at[2, k],
            fin_r.at[2, k],
            partner,
        )
        sums[p, i] = send_if(
            near,
            near_pending,
            cell(halves.at[0], p, i),
            cell(halves.at[0], p, i),
            fin_s.at[1, k],
            fin_r.at[1, k],
            core_peer,
        )
    y_cross = device(half, low, x, 1 - y, 1 - core)

    for p, i in cells:
        k = p * pieces + i
        wait_if(far, sums[p, i])
        wait_if(far, overs[p, i])

        @pl.when(far)
        def _():
            def one(r):
                c = at(i * size + r, chunk)
                tot_mine[c, wide[p]] = (
                    halves[0, c, wide[p]].astype(jnp.float32)
                    + halves[1, c, wide[p]].astype(jnp.float32)
                ).astype(jnp.bfloat16)

            over(0, size, one)

        mine_p, other_p = cell(tot_mine, p, i), cell(tot_other, p, i)
        third[p, i] = send_if(
            far, far_pending, mine_p, other_p, fin_s.at[3, k], fin_r.at[3, k], y_peer
        )
        fourth[p, i] = send_if(
            far, far_pending, mine_p, other_p, fin_s.at[4, k], fin_r.at[4, k], y_cross
        )
        shared[p, i] = send_if(
            far, far_pending, mine_p, mine_p, fin_s.at[5, k], fin_r.at[5, k], core_peer
        )

    def copy_out(start, p, i, src):
        def one(r):
            mean_ref[at(start + i * size + r, chunk), wide[p]] = src[
                at(i * size + r, chunk), wide[p]
            ]

        over(0, size, one)

    for p, i in cells:
        wait_if(near, shared[p, i])
        copy_out(y * mid, p, i, tot_mine)
    for p, i in cells:
        wait_if(far, third[p, i])
        wait_if(near, fourth[p, i])
        copy_out((1 - y) * mid, p, i, tot_other)
    for copy in pending:
        copy.wait_send()

    @pl.when(far)
    def _():
        for copy in far_pending:
            copy.wait_send()

    @pl.when(near)
    def _():
        for copy in near_pending:
            copy.wait_send()


def me_slot(core, low, x):
    return (core * 2 + low) * 2 + x


def shards(layer_input, queries, keys, targets, value_weight, outer_momentum):
    n = lax.axis_size("fsdp")
    replicas = lax.axis_size("replica")
    rows, columns = value_weight.shape
    steps, length, _ = layer_input.shape
    if rows % 512 or columns % (2 * HD) or n != 8 or replicas != 4 or length % 128 or steps != 2:
        return plain_shards(layer_input, queries, keys, targets, value_weight, outer_momentum)
    heads = columns // HD
    bf, f32 = jnp.bfloat16, jnp.float32
    dma = pltpu.SemaphoreType.DMA
    out = jax.ShapeDtypeStruct((rows, columns), bf)
    total_update = pl.pallas_call(
        round_kernel,
        out_shape=out,
        in_specs=[pl.BlockSpec(memory_space=pl.ANY)] * 5,
        out_specs=pl.BlockSpec(memory_space=pltpu.VMEM),
        scratch_shapes=[
            pltpu.VMEM((steps, n * length, rows), bf),
            pltpu.VMEM(queries.shape, bf),
            pltpu.VMEM(keys.shape, bf),
            pltpu.VMEM(targets.shape, bf),
            pltpu.VMEM((rows, columns), f32),
            pltpu.VMEM((2, rows, columns), bf),
            pltpu.VMEM((rows, columns), bf),
            pltpu.VMEM((4 * length, columns), f32),
            pltpu.VMEM((2, steps, heads, length, length), bf),
            pltpu.VMEM((2, steps, heads, length, HD), bf),
            pltpu.VMEM((steps, 4 * length, columns), bf),
            pltpu.VMEM((steps, 4 * length, columns), bf),
            pltpu.VMEM((steps, 4 * length, columns), bf),
            pltpu.VMEM((steps, 4, length, columns), bf),
            pltpu.VMEM((steps, n * length, columns), bf),
            pltpu.VMEM((steps, rows, columns), f32),
            pltpu.VMEM((rows, columns), f32),
            pltpu.VMEM((rows // 2, columns), bf),
            pltpu.VMEM((rows // 2, columns), bf),
            pltpu.VMEM((rows // 2, columns), f32),
            pltpu.VMEM((3, rows // 2, columns), bf),
            pltpu.VMEM((rows // 2, columns), bf),
            pltpu.VMEM((rows // 2, columns), bf),
            dma((steps, n)),
            dma((steps, n)),
            dma((2,)),
            dma((2,)),
            dma((steps, 2)),
            dma((steps, 2)),
            dma((steps, 2, 2)),
            dma((steps, 2, 2)),
            dma((steps, 4, 2)),
            dma((steps, 4, 2)),
            dma((steps, 4, 2)),
            dma((steps, 4, 2)),
            dma((steps, 4, 2)),
            dma((steps, 4, 2)),
            dma((6, 4)),
            dma((6, 4)),
            dma((4,)),
        ],
        compiler_params=pltpu.CompilerParams(collective_id=0, has_side_effects=True),
    )(layer_input, queries, keys, targets, value_weight)
    kept = (1.0 - inner_rate * decay_rate) ** steps
    mean_delta = (1.0 - kept) * value_weight + total_update.astype(f32) / replicas
    new_momentum = outer_mu * outer_momentum + mean_delta
    new_weight = value_weight - outer_rate * (mean_delta + outer_mu * new_momentum)
    return (new_weight, new_momentum)


def solution(mesh):
    in_specs = (
        P(None, ("replica", "fsdp"), None),
        P(None, ("replica", "fsdp"), None),
        P(None, ("replica", "fsdp"), None),
        P(None, ("replica", "fsdp"), None),
        P("fsdp", None),
        P("fsdp", None),
    )
    out_specs = (P("fsdp", None), P("fsdp", None))
    return jax.shard_map(shards, mesh=mesh, in_specs=in_specs, out_specs=out_specs, check_vma=False)
```

```python
import math

import jax
import jax.numpy as jnp
from jax import lax
from jax.experimental import pallas as pl
from jax.experimental.pallas import tpu as pltpu
from jax.sharding import PartitionSpec as P

D = 4096
QH = 32
KVH = 4
HD = 128


beta_one = 0.9
beta_two = 0.95
inner_rate = 0.05
decay_rate = 0.1
outer_rate = 0.7
outer_mu = 0.9


def plain_shards(layer_input, queries, keys, targets, value_weight, outer_momentum):
    inner_steps = layer_input.shape[0]
    length = layer_input.shape[1]
    columns = value_weight.shape[1]
    fsdp_count = lax.axis_size("fsdp")
    replicas = lax.axis_size("replica")
    tok_rep = length * fsdp_count
    group_size = QH // KVH
    adam_floor = math.sqrt(group_size / (tok_rep * D))
    by_features = lax.all_to_all(layer_input, "fsdp", split_axis=2, concat_axis=1, tiled=True)
    causal = jnp.arange(length)[:, None] >= jnp.arange(length)[None, :]
    weights_now = value_weight
    moment_one = jnp.zeros_like(value_weight)
    moment_two = jnp.zeros_like(value_weight)
    for step_index in range(inner_steps):
        inputs = layer_input[step_index]
        shard_bf = weights_now.astype(jnp.bfloat16)
        product = jnp.dot(
            inputs,
            lax.all_gather(shard_bf, "fsdp", axis=0, tiled=True),
            preferred_element_type=jnp.float32,
        )
        values = (product / math.sqrt(D)).astype(jnp.bfloat16)
        query_heads = queries[step_index].reshape(length, KVH, group_size, HD)
        key_heads = keys[step_index].reshape(length, KVH, HD)
        scores = jnp.einsum(
            "qgjd,kgd->gjqk", query_heads, key_heads, preferred_element_type=jnp.float32
        ) / math.sqrt(HD)
        scores = jnp.where(causal, scores, -1e30)
        highest = jnp.max(scores, axis=-1, keepdims=True)
        expd = jnp.exp(scores - highest)
        attention = (expd / jnp.sum(expd, axis=-1, keepdims=True)).astype(jnp.bfloat16)
        attended = jnp.einsum(
            "gjqk,kgd->qgjd",
            attention,
            values.reshape(length, KVH, HD),
            preferred_element_type=jnp.float32,
        ).reshape(length, QH * HD)
        out_grad = ((attended - targets[step_index].astype(jnp.float32)) / tok_rep).astype(
            jnp.bfloat16
        )
        value_grad = (
            jnp.einsum(
                "gjqk,qgjd->kgd",
                attention,
                out_grad.reshape(length, KVH, group_size, HD),
                preferred_element_type=jnp.float32,
            )
            .reshape(length, columns)
            .astype(jnp.bfloat16)
        )
        step_features = by_features[step_index]
        gradient = lax.dot_general(
            step_features,
            lax.all_gather(value_grad, "fsdp", axis=0, tiled=True),
            (((0,), (0,)), ((), ())),
            preferred_element_type=jnp.float32,
        ) / math.sqrt(D)
        moment_one = beta_one * moment_one + (1.0 - beta_one) * gradient
        moment_two = beta_two * moment_two + (1.0 - beta_two) * gradient * gradient
        corrected_one = moment_one / (1.0 - beta_one ** (step_index + 1))
        corrected_two = moment_two / (1.0 - beta_two ** (step_index + 1))
        weights_now = weights_now - inner_rate * (
            corrected_one / (jnp.sqrt(corrected_two) + adam_floor) + decay_rate * weights_now
        )
    total_delta = lax.psum(value_weight - weights_now, "replica")
    mean_delta = total_delta / replicas
    new_momentum = outer_mu * outer_momentum + mean_delta
    new_weight = value_weight - outer_rate * (mean_delta + outer_mu * new_momentum)
    return (new_weight, new_momentum)


MESH = pl.DeviceIdType.MESH


def round_kernel(
    x_ref,
    q_ref,
    k_ref,
    t_ref,
    w_ref,
    mean_ref,
    feat,
    q_buf,
    k_buf,
    t_buf,
    w_buf,
    wb,
    w_now,
    own_part,
    mat,
    base,
    pair_out,
    pair_in,
    red_out,
    red_in,
    vgrad,
    grad,
    first_update,
    sy_out,
    sy_in,
    s_own,
    halves,
    tot_mine,
    tot_other,
    in_s,
    in_r,
    w_s,
    w_r,
    mat_s,
    mat_r,
    pair_s,
    pair_r,
    red_s,
    red_r,
    ag_s,
    ag_r,
    fw_s,
    fw_r,
    fin_s,
    fin_r,
    load_s,
):
    steps, length, _ = x_ref.shape
    rows, columns = w_ref.shape
    parts = 2
    width = columns // parts
    wide = [slice(p * width, (p + 1) * width) for p in range(parts)]
    heads = columns // HD
    group = QH // KVH
    quad = 4 * length
    tok_rep = 2 * quad
    adam_floor = math.sqrt(group / (tok_rep * D))
    shrink = 1.0 - inner_rate * decay_rate
    me = lax.axis_index("fsdp")
    rep = lax.axis_index("replica")
    x = me % 2
    low = (me // 2) % 2
    half = me // 4
    y = rep // 2
    core = rep % 2
    sel = (half + core) % 2
    far = sel == 1
    near = sel == 0
    beside = jnp.logical_and(far, low != half)
    outer = jnp.logical_and(far, low == half)

    def device(h, l, xx, yy, cc):
        return {"replica": yy * 2 + cc, "fsdp": (h * 2 + l) * 2 + xx}

    core_peer = device(half, low, x, y, 1 - core)
    y_peer = device(half, low, x, 1 - y, core)
    partner = device(core, low, x, y, half)

    def mate(a, b):
        return device(half, (low + a) % 2, (x + b) % 2, y, core)

    def offset(a, b):
        return (((low + a) % 2) * 2 + (x + b) % 2) * length

    quads = [(1, 1), (0, 1), (1, 0), (0, 0)]

    def at(start, size):
        return pl.ds(pl.multiple_of(start, 32), size)

    loads = {}

    def load(i, src, dst):
        loads[i] = pltpu.make_async_copy(src, dst, load_s.at[i])
        loads[i].start()

    barrier = pltpu.get_barrier_semaphore()
    count = 0
    for dh in range(2):
        for dl in range(2):
            for dx in range(2):
                for dc in range(2):
                    if dh + dl + dx + dc:
                        peer = device(
                            (half + dh) % 2, (low + dl) % 2, (x + dx) % 2, y, (core + dc) % 2
                        )
                        pl.semaphore_signal(barrier, inc=1, device_id=peer, device_id_type=MESH)
                        count += 1
    for dc in range(2):
        peer = device(half, low, x, 1 - y, (core + dc) % 2)
        pl.semaphore_signal(barrier, inc=1, device_id=peer, device_id_type=MESH)
    load(0, w_ref, w_buf)
    load(1, q_ref, q_buf)
    load(2, k_ref, k_buf)
    load(3, t_ref, t_buf)
    pl.semaphore_wait(barrier, count + 2)

    pending, far_pending, near_pending = [], [], []

    def remote(src, dst, ssem, rsem, peer):
        return pltpu.make_async_remote_copy(
            src_ref=src,
            dst_ref=dst,
            send_sem=ssem,
            recv_sem=rsem,
            device_id=peer,
            device_id_type=MESH,
        )

    def send(*args):
        copy = remote(*args)
        copy.start()
        pending.append(copy)
        return copy

    def send_if(cond, keep, *args):
        copy = remote(*args)

        @pl.when(cond)
        def _():
            copy.start()

        keep.append(copy)
        return copy

    def wait_if(cond, copy):
        @pl.when(cond)
        def _():
            copy.wait_recv()

    def send_inputs(s, picks, cond=None, keep=None):
        for a, b, dc in picks:
            l2, x2, c2 = (low + a) % 2, (x + b) % 2, (core + dc) % 2
            i = a * 4 + b * 2 + dc
            src = x_ref.at[
                s, :, pl.ds(pl.multiple_of(((c2 * 2 + l2) * 2 + x2) * rows, 128), rows)
            ]
            dst = feat.at[s, at(me * length, length)]
            args = (src, dst, in_s.at[s, i], in_r.at[s, me], device(core, l2, x2, y, c2))
            if i and cond is None:
                send(*args)
            elif i:
                send_if(cond, keep, *args)
            else:
                if cond is not near:
                    send_if(far if cond is None else cond, far_pending if cond is None else keep, *args)
                if cond is None or cond is near:

                    @pl.when(near)
                    def _():
                        pltpu.make_async_copy(src, dst, in_r.at[s, me]).start()

    def wait_input(s, j):
        slot = feat.at[s, at(j * length, length)]
        remote(slot, slot, in_s.at[s, 0], in_r.at[s, j], core_peer).wait_recv()

    causal = lax.broadcasted_iota(jnp.int32, (length, length), 0) >= lax.broadcasted_iota(
        jnp.int32, (length, length), 1
    )

    def attention_of(s):
        def one(g, carry):
            keys = k_buf[s, :, pl.ds(pl.multiple_of(g * HD, HD), HD)]
            both = jnp.zeros((length, length + HD), jnp.float32)
            for j in range(group):
                cols = pl.ds(pl.multiple_of((g * group + j) * HD, HD), HD)
                scores = lax.dot_general(
                    q_buf[s, :, cols],
                    keys,
                    (((1,), (1,)), ((), ())),
                    preferred_element_type=jnp.float32,
                ) / math.sqrt(HD)
                scores = jnp.where(causal, scores, -1e30)
                highest = jnp.max(scores, axis=-1, keepdims=True)
                expd = jnp.exp(scores - highest)
                att = (expd / jnp.sum(expd, axis=-1, keepdims=True)).astype(jnp.bfloat16)
                both += lax.dot_general(
                    att,
                    jnp.concatenate([att, t_buf[s, :, cols]], axis=1),
                    (((0,), (0,)), ((), ())),
                    preferred_element_type=jnp.float32,
                )
            mat[0, s, g] = both[:, :length].astype(jnp.bfloat16)
            base[0, s, g] = both[:, length:].astype(jnp.bfloat16)
            return carry

        lax.fori_loop(0, heads, one, 0)

    def send_products(s, cond, keep):
        return [
            send_if(cond, keep, buf.at[0, s], buf.at[1, s], mat_s.at[s, i], mat_r.at[s, i], partner)
            for i, buf in enumerate((mat, base))
        ]

    chunk = 64

    def over(start, size, body):
        def step(i, carry):
            body(i * chunk)
            return carry

        lax.fori_loop(0, size // chunk, step, 0)

    order = [(a, b, dc) for a, b in quads for dc in (1, 0)]
    loads[0].wait()

    def cast_weights(r):
        wb[0, at(r, chunk), :] = w_buf[at(r, chunk), :].astype(jnp.bfloat16)

    over(0, rows, cast_weights)
    mid = rows // 2
    w_mine = at(y * mid, mid)
    w_cross = send_if(
        far, far_pending, wb.at[0, w_mine], wb.at[1, w_mine], w_s.at[0], w_r.at[0], partner
    )
    send_inputs(0, order)
    for s in range(1, steps):
        pass
    for i in (1, 2, 3):
        loads[i].wait()
    wait_if(far, w_cross)
    w_relay = send_if(
        far, far_pending, wb.at[1, w_mine], wb.at[1, w_mine], w_s.at[1], w_r.at[1], y_peer
    )
    attention_of(0)
    products = [send_products(0, far, far_pending)]
    for s in range(1, steps):
        send_inputs(s, order, beside, far_pending)
        send_inputs(s, order, near, near_pending)
    wait_if(far, w_relay)

    def weights(s, p):
        return wb[sel, :, wide[p]] if s == 0 else w_now[:, wide[p]]

    sides = ((half * quad, near, far, near_pending, far_pending),
             ((1 - half) * quad, far, near, far_pending, near_pending))
    slot = at(me_slot(core, low, x) * length, length)
    for s in range(steps):

        def scatter(start, taker, giver, keep, keep_giver):
            for a, b in quads:
                wait_input(s, start // length + ((low + a) % 2) * 2 + (x + b) % 2)
            pairs, reds = {}, {}
            for p in range(parts):
                for a in (1, 0):
                    first = ((low + a) % 2) * 2 * length
                    span = at(first, 2 * length)
                    part = jnp.dot(
                        feat[s, at(start + first, 2 * length)],
                        weights(s, p),
                        preferred_element_type=jnp.float32,
                    )
                    own_part[span, wide[p]] = part

                    @pl.when(giver)
                    def _():
                        pair_out[s, span, wide[p]] = part.astype(jnp.bfloat16)

                    pairs[a, p] = send_if(
                        giver,
                        keep_giver,
                        pair_out.at[s, span, wide[p]],
                        pair_in.at[s, span, wide[p]],
                        pair_s.at[s, a, p],
                        pair_r.at[s, a, p],
                        core_peer,
                    )
            for p in range(parts):
                for a in (1, 0):
                    span = at(((low + a) % 2) * 2 * length, 2 * length)
                    wait_if(taker, pairs[a, p])

                    @pl.when(taker)
                    def _():
                        red_out[s, span, wide[p]] = (
                            own_part[span, wide[p]]
                            + pair_in[s, span, wide[p]].astype(jnp.float32)
                        ).astype(jnp.bfloat16)

                    for b in (1, 0):
                        if a + b:
                            reds[a, b, p] = send_if(
                                taker,
                                keep,
                                red_out.at[s, at(offset(a, b), length), wide[p]],
                                red_in.at[s, a * 2 + b, :, wide[p]],
                                red_s.at[s, a * 2 + b, p],
                                red_r.at[s, a * 2 + b, p],
                                mate(a, b),
                            )
            return reds

        def reduce(reds, start, taker, giver, keep, keep_giver):
            gathers, passes = {}, {}
            for p in range(parts):
                for a, b in quads[:3]:
                    wait_if(taker, reds[a, b, p])

                @pl.when(taker)
                def _():
                    summed = red_out[s, at(offset(0, 0), length), wide[p]].astype(jnp.float32)
                    for a, b in quads[:3]:
                        summed = summed + red_in[s, a * 2 + b, :, wide[p]].astype(jnp.float32)
                    values = (summed / math.sqrt(D)).astype(jnp.bfloat16)
                    for i in range(width // HD):
                        g = p * (width // HD) + i
                        part = values[:, i * HD : (i + 1) * HD]
                        vg = jnp.dot(mat[sel, s, g], part, preferred_element_type=jnp.float32)
                        vg = (vg - base[sel, s, g].astype(jnp.float32)) / tok_rep
                        vgrad[s, slot, g * HD : (g + 1) * HD] = vg.astype(jnp.bfloat16)

                block = vgrad.at[s, slot, wide[p]]
                for a, b in quads[:3]:
                    i = a * 2 + b
                    gathers[a, b, p] = send_if(
                        taker, keep, block, block, ag_s.at[s, i, p], ag_r.at[s, i, p], mate(a, b)
                    )
                passes[0, 0, p] = send_if(
                    taker, keep, block, block, fw_s.at[s, 0, p], fw_r.at[s, 0, p], core_peer
                )
            return gathers, passes

        def forward(copies, p, start, taker, giver, keep, keep_giver):
            gathers, passes = copies
            for a, b in quads[2::-1]:
                wait_if(taker, gathers[a, b, p])
                i = a * 2 + b
                block = vgrad.at[s, at(start + offset(a, b), length), wide[p]]
                passes[a, b, p] = send_if(
                    taker, keep, block, block, fw_s.at[s, i, p], fw_r.at[s, i, p], core_peer
                )

        def add_quad(copies, first, p, start, taker, giver, keep, keep_giver):
            for a, b in quads[::-1]:
                wait_if(giver, copies[1][a, b, p])
            term = lax.dot_general(
                feat[s, at(start, quad)],
                vgrad[s, at(start, quad), wide[p]],
                (((0,), (0,)), ((), ())),
                preferred_element_type=jnp.float32,
            )
            if first:
                grad[s, :, wide[p]] = term
            else:
                grad[s, :, wide[p]] += term

        near_reds = scatter(*sides[0])
        if s:
            products.append(send_products(s, far, far_pending))
        near_copies = reduce(near_reds, *sides[0])
        if s + 1 < steps:
            attention_of(s + 1)
        far_reds = scatter(*sides[1])
        if s + 1 < steps:
            send_inputs(s + 1, order[:4], outer, [])
        for p in range(parts):
            forward(near_copies, p, *sides[0])
        for p in range(parts):
            add_quad(near_copies, True, p, *sides[0])
        for copy in products[s]:
            wait_if(far, copy)
        far_copies = reduce(far_reds, *sides[1])
        if s + 1 < steps:
            send_inputs(s + 1, order[4:], outer, [])
            for p in range(parts):
                forward(far_copies, p, *sides[1])
            for p in range(parts):
                add_quad(far_copies, False, p, *sides[1])

        def adam(r, cols, keep):
            c = at(r, chunk)
            one, two = 0.0, 0.0
            for i in range(s + 1):
                gradient = grad[i, c, cols] / math.sqrt(D)
                one = beta_one * one + (1.0 - beta_one) * gradient
                two = beta_two * two + (1.0 - beta_two) * gradient * gradient
            fixed_one = one / (1.0 - beta_one ** (s + 1))
            fixed_two = two / (1.0 - beta_two ** (s + 1))
            keep(c, fixed_one / (jnp.sqrt(fixed_two) + adam_floor))

        if s + 1 < steps:

            def keep(c, update):
                before = wb[sel, c, :].astype(jnp.float32)
                first_update[c, :] = update
                w_now[c, :] = (before * shrink - inner_rate * update).astype(jnp.bfloat16)

            over(0, rows, lambda r: adam(r, slice(None), keep))

    pieces = 2
    size = mid // pieces
    crosses, sums, overs, shared, third, fourth = {}, {}, {}, {}, {}, {}
    cells = [(p, i) for p in range(parts) for i in range(pieces)]

    def moved(c, cols, update):
        return inner_rate * (shrink * first_update[c, cols] + update)

    def cell(ref, p, i):
        return ref.at[at(i * size, size), wide[p]]

    for p in range(parts):
        forward(far_copies, p, *sides[1])
        add_quad(far_copies, False, p, *sides[1])
        for i in range(pieces):

            def out_rows(r):
                def put(c, update):
                    sy_out[at(i * size + r, chunk), wide[p]] = moved(c, wide[p], update).astype(
                        jnp.bfloat16
                    )

                adam((1 - y) * mid + i * size + r, wide[p], put)

            over(0, size, out_rows)
            k = p * pieces + i
            crosses[p, i] = send(
                cell(sy_out, p, i), cell(sy_in, p, i), fin_s.at[0, k], fin_r.at[0, k], y_peer
            )
    for p in range(parts):

        def own_rows(r):
            def put(c, update):
                s_own[at(r, chunk), wide[p]] = moved(c, wide[p], update)

            adam(y * mid + r, wide[p], put)

        over(0, mid, own_rows)
    for p, i in cells:
        k = p * pieces + i
        crosses[p, i].wait_recv()

        def join(r):
            c = at(i * size + r, chunk)
            halves[2 * sel, c, wide[p]] = (
                s_own[c, wide[p]] + sy_in[c, wide[p]].astype(jnp.float32)
            ).astype(jnp.bfloat16)

        over(0, size, join)
        overs[p, i] = send_if(
            far,
            far_pending,
            cell(halves.at[2], p, i),
            cell(halves.at[1], p, i),
            fin_s.at[2, k],
            fin_r.at[2, k],
            partner,
        )
        sums[p, i] = send_if(
            near,
            near_pending,
            cell(halves.at[0], p, i),
            cell(halves.at[0], p, i),
            fin_s.at[1, k],
            fin_r.at[1, k],
            core_peer,
        )
    y_cross = device(half, low, x, 1 - y, 1 - core)

    for p, i in cells:
        k = p * pieces + i
        wait_if(far, sums[p, i])
        wait_if(far, overs[p, i])

        @pl.when(far)
        def _():
            def one(r):
                c = at(i * size + r, chunk)
                tot_mine[c, wide[p]] = (
                    halves[0, c, wide[p]].astype(jnp.float32)
                    + halves[1, c, wide[p]].astype(jnp.float32)
                ).astype(jnp.bfloat16)

            over(0, size, one)

        mine_p, other_p = cell(tot_mine, p, i), cell(tot_other, p, i)
        third[p, i] = send_if(
            far, far_pending, mine_p, other_p, fin_s.at[3, k], fin_r.at[3, k], y_peer
        )
        fourth[p, i] = send_if(
            far, far_pending, mine_p, other_p, fin_s.at[4, k], fin_r.at[4, k], y_cross
        )
        shared[p, i] = send_if(
            far, far_pending, mine_p, mine_p, fin_s.at[5, k], fin_r.at[5, k], core_peer
        )

    def copy_out(start, p, i, src):
        def one(r):
            mean_ref[at(start + i * size + r, chunk), wide[p]] = src[
                at(i * size + r, chunk), wide[p]
            ]

        over(0, size, one)

    for p, i in cells:
        wait_if(near, shared[p, i])
        copy_out(y * mid, p, i, tot_mine)
    for p, i in cells:
        wait_if(far, third[p, i])
        wait_if(near, fourth[p, i])
        copy_out((1 - y) * mid, p, i, tot_other)
    for copy in pending:
        copy.wait_send()

    @pl.when(far)
    def _():
        for copy in far_pending:
            copy.wait_send()

    @pl.when(near)
    def _():
        for copy in near_pending:
            copy.wait_send()


def me_slot(core, low, x):
    return (core * 2 + low) * 2 + x


def shards(layer_input, queries, keys, targets, value_weight, outer_momentum):
    n = lax.axis_size("fsdp")
    replicas = lax.axis_size("replica")
    rows, columns = value_weight.shape
    steps, length, _ = layer_input.shape
    if rows % 512 or columns % (2 * HD) or n != 8 or replicas != 4 or length % 128 or steps != 2:
        return plain_shards(layer_input, queries, keys, targets, value_weight, outer_momentum)
    heads = columns // HD
    bf, f32 = jnp.bfloat16, jnp.float32
    dma = pltpu.SemaphoreType.DMA
    out = jax.ShapeDtypeStruct((rows, columns), bf)
    total_update = pl.pallas_call(
        round_kernel,
        out_shape=out,
        in_specs=[pl.BlockSpec(memory_space=pl.ANY)] * 5,
        out_specs=pl.BlockSpec(memory_space=pltpu.VMEM),
        scratch_shapes=[
            pltpu.VMEM((steps, n * length, rows), bf),
            pltpu.VMEM(queries.shape, bf),
            pltpu.VMEM(keys.shape, bf),
            pltpu.VMEM(targets.shape, bf),
            pltpu.VMEM((rows, columns), f32),
            pltpu.VMEM((2, rows, columns), bf),
            pltpu.VMEM((rows, columns), bf),
            pltpu.VMEM((4 * length, columns), f32),
            pltpu.VMEM((2, steps, heads, length, length), bf),
            pltpu.VMEM((2, steps, heads, length, HD), bf),
            pltpu.VMEM((steps, 4 * length, columns), bf),
            pltpu.VMEM((steps, 4 * length, columns), bf),
            pltpu.VMEM((steps, 4 * length, columns), bf),
            pltpu.VMEM((steps, 4, length, columns), bf),
            pltpu.VMEM((steps, n * length, columns), bf),
            pltpu.VMEM((steps, rows, columns), f32),
            pltpu.VMEM((rows, columns), f32),
            pltpu.VMEM((rows // 2, columns), bf),
            pltpu.VMEM((rows // 2, columns), bf),
            pltpu.VMEM((rows // 2, columns), f32),
            pltpu.VMEM((3, rows // 2, columns), bf),
            pltpu.VMEM((rows // 2, columns), bf),
            pltpu.VMEM((rows // 2, columns), bf),
            dma((steps, n)),
            dma((steps, n)),
            dma((2,)),
            dma((2,)),
            dma((steps, 2)),
            dma((steps, 2)),
            dma((steps, 2, 2)),
            dma((steps, 2, 2)),
            dma((steps, 4, 2)),
            dma((steps, 4, 2)),
            dma((steps, 4, 2)),
            dma((steps, 4, 2)),
            dma((steps, 4, 2)),
            dma((steps, 4, 2)),
            dma((6, 4)),
            dma((6, 4)),
            dma((4,)),
        ],
        compiler_params=pltpu.CompilerParams(collective_id=0, has_side_effects=True),
    )(layer_input, queries, keys, targets, value_weight)
    kept = (1.0 - inner_rate * decay_rate) ** steps
    mean_delta = (1.0 - kept) * value_weight + total_update.astype(f32) / replicas
    new_momentum = outer_mu * outer_momentum + mean_delta
    new_weight = value_weight - outer_rate * (mean_delta + outer_mu * new_momentum)
    return (new_weight, new_momentum)


def solution(mesh):
    in_specs = (
        P(None, ("replica", "fsdp"), None),
        P(None, ("replica", "fsdp"), None),
        P(None, ("replica", "fsdp"), None),
        P(None, ("replica", "fsdp"), None),
        P("fsdp", None),
        P("fsdp", None),
    )
    out_specs = (P("fsdp", None), P("fsdp", None))
    return jax.shard_map(shards, mesh=mesh, in_specs=in_specs, out_specs=out_specs, check_vma=False)
```
